32 devices in a mesh: gx: 4 (over y, x), gy: 4 (over z), gz: 2 (over core).
Axes of the slice: x: 2, y: 2, z: 4, core: 2. Of those that a mesh axis runs over, the one named last changes fastest.
Arguments:
- gas_pos: float32 [3, 4, 4, 2, 2048], P(None, 'gx', 'gy', 'gz'), may hold values from 0 to 1
- gas_mass: float32 [4, 4, 2, 2048], P('gx', 'gy', 'gz'), may hold values from 0.2 to 5
- source_pos: float32 [3, 4, 4, 2, 2048], P(None, 'gx', 'gy', 'gz'), may hold values from 0 to 1
- source_radius: float32 [4, 4, 2, 2048], P('gx', 'gy', 'gz'), may hold values from 0.25 to 1
- source_yield: float32 [2, 4, 4, 2, 2048], P(None, 'gx', 'gy', 'gz'), may hold values from 1 to 30
- source_momentum: float32 [3, 4, 4, 2, 2048], P(None, 'gx', 'gy', 'gz'), may hold values from -180 to 180
- source_tiles: int32 [4, 4, 2, 16, 8], P('gx', 'gy', 'gz'), may hold values from 0 to 431, as said below
- source_count: int32 [4, 4, 2], P('gx', 'gy', 'gz'), may hold values from 1 to 2048, as said below
Outputs:
- gas_gain: float32 [5, 4, 4, 2, 2048], P(None, 'gx', 'gy', 'gz')
The draws below stay inside these ranges and needn't reach their ends.
Inputs may be any that keep to these rules, and one draw needn't show every extreme that they name: `source_tiles`: the 8 tiles of one block lie one in each of the 8 domains around one corner of the block's domain (that domain among them), in increasing order. Over all blocks of one domain, at most 8 distinct listed tiles lie in any one neighbouring slot. `source_count`: some domain holds 2048 live sources in every draw.
All inputs are finite; a program needn't handle non-finite values.
Results may differ from the reference program's by a relative error of at most 0.0003.
Values sent between devices are 32-bit elements; how exact they have to be, the bound alone decides.
A program may use at most 64 MiB of HBM per device.

```python
import math
import jax
import jax.numpy as jnp
from jax import lax

GAS = 2048
SRC_BLOCKS = 16
TILES_LISTED = 8
GAS_TILES = 16
SOURCES = 2048
DOM_X = 4
DOM_Y = 4
DOM_Z = 2


def feedback_layout(key):
    base = jax.random.fold_in(key, 2024)
    streams = jax.random.split(base, 6)
    domains = DOM_X * DOM_Y * DOM_Z
    capacity = GAS_TILES // 2
    dom_ids = jnp.arange(domains, dtype=jnp.int32)
    counts = jax.random.randint(streams[0], (domains,), 1, SOURCES + 1)
    chosen = jax.random.randint(streams[1], (), 0, domains)
    counts = jnp.where(dom_ids == chosen, SOURCES, counts).astype(jnp.int32)
    scores = jax.random.randint(streams[2], (domains, 27, GAS_TILES), 0, 262144)
    scores = scores * GAS_TILES + jnp.arange(GAS_TILES, dtype=jnp.int32)[None, None, :]
    candidates = lax.top_k(scores, capacity)[1].astype(jnp.int32)
    corners = jax.random.randint(streams[3], (domains, SRC_BLOCKS), 0, 8)
    forced = jax.random.randint(streams[4], (), 0, 8)
    block_ids = jnp.arange(SRC_BLOCKS, dtype=jnp.int32)
    pinned = (dom_ids[:, None] == chosen) & (block_ids[None, :] < capacity)
    corners = jnp.where(pinned, forced, corners).astype(jnp.int32)
    rotate = jax.random.randint(streams[5], (domains, 27), 0, capacity)
    octant = jnp.arange(8, dtype=jnp.int32)
    sign_x = 2 * (corners // 4) - 1
    sign_y = 2 * (corners // 2 % 2) - 1
    sign_z = 2 * (corners % 2) - 1
    slots = 9 * (sign_x[:, :, None] * (octant // 4)[None, None, :] + 1)
    slots = slots + 3 * (sign_y[:, :, None] * (octant // 2 % 2)[None, None, :] + 1)
    slots = slots + (sign_z[:, :, None] * (octant % 2)[None, None, :] + 1)
    slot_flat = slots.reshape(domains, SRC_BLOCKS * 8)
    turned = jnp.take_along_axis(rotate, slot_flat, axis=1).reshape(domains, SRC_BLOCKS, 8)
    member = (block_ids[None, :, None] + turned) % capacity
    where_flat = (slots * capacity + member).reshape(domains, SRC_BLOCKS * 8)
    tiles = jnp.take_along_axis(candidates.reshape(domains, 27 * capacity), where_flat, axis=1)
    listed = slots * GAS_TILES + tiles.reshape(domains, SRC_BLOCKS, 8)
    listed = jnp.sort(listed, axis=-1).astype(jnp.int32)
    return (listed.reshape(DOM_X, DOM_Y, DOM_Z, SRC_BLOCKS, 8), counts.reshape(DOM_X, DOM_Y, DOM_Z))


def draw_source_tiles(key, part):
    return feedback_layout(key)[0]


def draw_source_count(key, part):
    return feedback_layout(key)[1]


def level_of(own_key, shape, shards, least, high):
    factor_of, own = 1.0, jax.random.fold_in(own_key, 6)
    for axis_at, shards_of in shards:
        draws = jnp.exp(jax.random.uniform(jax.random.fold_in(own, axis_at), (shards_of,), jnp.float32, least / len(shards), high / len(shards)))
        factor_of = factor_of * jnp.repeat(draws, shape[axis_at] // shards_of).reshape([-1 if axis == axis_at else 1 for axis in range(len(shape))])
    return factor_of


def normal_values(rng, extent, scale, bound, cuts=(), kind=jnp.bfloat16):
    level = level_of(rng, extent, cuts, -0.22, 0.18) if cuts else 1.0
    drawn = jax.random.normal(rng, extent, jnp.float32) * scale * level
    return jnp.minimum(jnp.maximum(drawn, -bound), bound).astype(kind)


def setup_inputs(seed: int = 0) -> dict:
    key_of = jax.random.split(jax.random.key(seed), 9)
    gas_pos = jnp.clip(1.0 * jax.random.uniform(key_of[0], (3, DOM_X, DOM_Y, DOM_Z, GAS), jnp.float32) ** level_of(key_of[0], (3, DOM_X, DOM_Y, DOM_Z, GAS), ((1, 4), (2, 4), (3, 2)), -0.2, 0.2), 0.0, 1.0)
    gas_mass = jnp.clip(jnp.exp(math.log(5.0) - 3.218876 * jax.random.uniform(key_of[1], (DOM_X, DOM_Y, DOM_Z, GAS), jnp.float32) ** level_of(key_of[1], (DOM_X, DOM_Y, DOM_Z, GAS), ((0, 4), (1, 4), (2, 2)), -0.2, 0.2)), 0.2, 5.0)
    source_pos = jnp.clip(1.0 * jax.random.uniform(key_of[2], (3, DOM_X, DOM_Y, DOM_Z, SOURCES), jnp.float32) ** level_of(key_of[2], (3, DOM_X, DOM_Y, DOM_Z, SOURCES), ((1, 4), (2, 4), (3, 2)), -0.2, 0.2), 0.0, 1.0)
    source_radius = jnp.clip(jnp.exp(math.log(1.0) - 1.3862944 * jax.random.uniform(key_of[3], (DOM_X, DOM_Y, DOM_Z, SOURCES), jnp.float32) ** level_of(key_of[3], (DOM_X, DOM_Y, DOM_Z, SOURCES), ((0, 4), (1, 4), (2, 2)), -0.2, 0.2)), 0.25, 1.0)
    source_yield = jnp.clip(jnp.exp(math.log(30.0) - 3.4011974 * jax.random.uniform(key_of[4], (2, DOM_X, DOM_Y, DOM_Z, SOURCES), jnp.float32) ** level_of(key_of[4], (2, DOM_X, DOM_Y, DOM_Z, SOURCES), ((1, 4), (2, 4), (3, 2)), -0.2, 0.2)), 1.0, 30.0)
    source_momentum = normal_values(key_of[5], (3, DOM_X, DOM_Y, DOM_Z, SOURCES), 30.0, 180.0, ((1, 4), (2, 4), (3, 2)), jnp.float32)
    source_tiles = draw_source_tiles(jax.random.fold_in(key_of[8], 71), 0)
    source_count = draw_source_count(jax.random.fold_in(key_of[8], 71), 0)
    return dict(gas_pos=gas_pos, gas_mass=gas_mass, source_pos=source_pos, source_radius=source_radius, source_yield=source_yield, source_momentum=source_momentum, source_tiles=source_tiles, source_count=source_count)


def block_deposit(near, tile_ids, source_xyz, inv_square, load, live, tiles_each):
    picked = jnp.take(near, tile_ids, axis=1)
    slot = tile_ids // tiles_each
    shifts = jnp.stack([slot // 9 - 1, (slot // 3) % 3 - 1, slot % 3 - 1]).astype(near.dtype)
    gas_xyz = (picked[0:3] + shifts[:, :, None]).reshape(3, -1)
    masses = picked[3].reshape(-1)
    dist_sq = jnp.square(gas_xyz[0][None, :] - source_xyz[0][:, None])
    dist_sq = dist_sq + jnp.square(gas_xyz[1][None, :] - source_xyz[1][:, None])
    dist_sq = dist_sq + jnp.square(gas_xyz[2][None, :] - source_xyz[2][:, None])
    weight = masses[None, :] / jnp.square(1.0 + dist_sq * inv_square[:, None])
    norm_sum = jnp.sum(weight, axis=1)
    coeffs = load * (live / norm_sum)[None, :]
    moved = jnp.dot(coeffs, weight, precision=lax.Precision.HIGHEST, preferred_element_type=jnp.float32)
    return moved.reshape(load.shape[0], tile_ids.shape[0], 128)


def reference(gas_pos, gas_mass, source_pos, source_radius, source_yield, source_momentum, source_tiles, source_count):
    gas_all = jnp.concatenate([gas_pos, gas_mass[None]], axis=0)
    load_all = jnp.concatenate([source_yield[0:1], source_momentum, source_yield[1:2]], axis=0)
    inv_all = (1.0 / jnp.square(source_radius))[None]
    zero = jnp.zeros((), jnp.int32)
    gain_init = jnp.zeros((5, DOM_X, DOM_Y, DOM_Z, GAS), jnp.float32)

    def per_device(gain, flat):
        ix = (flat // (DOM_Y * DOM_Z)).astype(jnp.int32)
        iy = ((flat // DOM_Z) % DOM_Y).astype(jnp.int32)
        iz = (flat % DOM_Z).astype(jnp.int32)
        starts = []
        for slot in range(27):
            sx = ((ix + slot // 9 - 1) % DOM_X).astype(jnp.int32)
            sy = ((iy + (slot // 3) % 3 - 1) % DOM_Y).astype(jnp.int32)
            sz = ((iz + slot % 3 - 1) % DOM_Z).astype(jnp.int32)
            starts.append((zero, sx, sy, sz, zero))
        pieces = [lax.dynamic_slice(gas_all, start, (4, 1, 1, 1, GAS)).reshape(4, GAS) for start in starts]
        near = jnp.stack(pieces, axis=1).reshape(4, 27 * GAS_TILES, 128)

        def own_rows(array):
            rows = lax.dynamic_slice(array, (zero, ix, iy, iz, zero), (array.shape[0], 1, 1, 1, SOURCES))
            return rows.reshape(array.shape[0], SRC_BLOCKS, 128)

        source_xyz = own_rows(source_pos)
        loads = own_rows(load_all)
        inv_sq = own_rows(inv_all)[0]
        tile_table = lax.dynamic_slice(source_tiles, (ix, iy, iz, zero, zero), (1, 1, 1, SRC_BLOCKS, TILES_LISTED)).reshape(SRC_BLOCKS, TILES_LISTED)
        live_count = lax.dynamic_slice(source_count, (ix, iy, iz), (1, 1, 1)).reshape(())
        used_blocks = ((live_count + 127) // 128).astype(jnp.int32)

        def add_block(block_idx, acc):
            live = (block_idx * 128 + jnp.arange(128, dtype=jnp.int32) < live_count).astype(gas_all.dtype)
            ids = lax.dynamic_index_in_dim(tile_table, block_idx, 0, keepdims=False)
            xyz_rows = lax.dynamic_index_in_dim(source_xyz, block_idx, 1, keepdims=False)
            inv_rows = lax.dynamic_index_in_dim(inv_sq, block_idx, 0, keepdims=False)
            load_rows = lax.dynamic_index_in_dim(loads, block_idx, 1, keepdims=False)
            moved = block_deposit(near, ids, xyz_rows, inv_rows, load_rows, live, GAS_TILES)
            return acc.at[:, ids].add(moved)

        acc_init = jnp.zeros((5, 27 * GAS_TILES, 128), jnp.float32)
        acc = lax.fori_loop(zero, used_blocks, add_block, acc_init)
        spread = acc.reshape(5, 27, GAS)
        for slot in range(27):
            current = lax.dynamic_slice(gain, starts[slot], (5, 1, 1, 1, GAS))
            gain = lax.dynamic_update_slice(gain, current + spread[:, slot].reshape(5, 1, 1, 1, GAS), starts[slot])
        return gain, None

    gain, unused_all = lax.scan(per_device, gain_init, jnp.arange(DOM_X * DOM_Y * DOM_Z, dtype=jnp.int32))
    return gain / gas_mass[None]
```

```python
import functools
import math

import jax
import jax.numpy as jnp
from jax import lax
from jax.experimental import pallas as pl
from jax.experimental.pallas import tpu as pltpu
from jax.sharding import PartitionSpec as P


def kinds(count):
    return min(count, 3)


def kind_of(offset, count):
    if count >= 3:
        return offset + 1
    if count == 2:
        return jnp.abs(offset)
    return offset * 0


def own_kind(count):
    return 1 if count >= 3 else 0


def steps_of(count):
    if count >= 3:
        return ((0, -1), (2, 1))
    return ((1, 1),) if count == 2 else ()


MESH = pl.DeviceIdType.MESH
LIMIT = 24 * 1024 * 1024


def shifted(axis, count, step):
    return lax.rem(lax.axis_index(axis) + step + count, count)


def columns_of(sizes):
    nx, ny, _ = sizes
    choices_x = steps_of(nx) + ((own_kind(nx), 0),)
    choices_y = ((own_kind(ny), 0),) + steps_of(ny)
    return [
        ((i, j), {"gx": shifted("gx", nx, dx), "gy": shifted("gy", ny, dy)})
        for i, dx in choices_x
        for j, dy in choices_y
        if dx or dy
    ]


def cores_of(sizes):
    return [(k, {"gz": shifted("gz", sizes[2], dz)}) for k, dz in steps_of(sizes[2])]


def greet(sizes):
    barrier = pltpu.get_barrier_semaphore()
    peers = columns_of(sizes) + cores_of(sizes)
    for _, device in peers:
        pl.semaphore_signal(barrier, inc=1, device_id=device, device_id_type=MESH)
    if peers:
        pl.semaphore_wait(barrier, len(peers))


def facing(kind, count):
    return 2 - kind if count >= 3 else kind


def spread_kernel(sizes, pos, mass, near, local_sem, send_sem, recv_sem):
    nx, ny, nz = sizes
    own = tuple(own_kind(n) for n in sizes)

    def place(i, j, k):
        return (i * kinds(ny) + j) * kinds(nz) + k

    home = place(*own)
    first = pltpu.make_async_copy(pos, near.at[home, pl.ds(0, 3)], local_sem.at[0])
    second = pltpu.make_async_copy(mass, near.at[home, pl.ds(3, 1)], local_sem.at[1])
    first.start()
    second.start()
    greet(sizes)
    first.wait()
    second.wait()
    copies = {}

    def send(slot, there, device):
        target = place(*there)
        copy = pltpu.make_async_remote_copy(
            src_ref=near.at[place(*slot)],
            dst_ref=near.at[target],
            send_sem=send_sem.at[target],
            recv_sem=recv_sem.at[target],
            device_id=device,
            device_id_type=MESH,
        )
        copy.start()
        copies[there] = copy

    def to_cores(i, j):
        for k, device in cores_of(sizes):
            send((i, j, own[2]), (i, j, facing(k, nz)), device)

    columns = columns_of(sizes)
    for (i, j), device in columns:
        send(own, (facing(i, nx), facing(j, ny), own[2]), device)
    to_cores(own[0], own[1])
    across = [at for at, _ in columns if at[0] != own[0]]
    along = [at for at, _ in columns if at[0] == own[0]]
    for i, j in along + across:
        copies[i, j, own[2]].wait_recv()
        to_cores(i, j)
    for i, j in [own[:2]] + along + across:
        for k, _ in steps_of(nz):
            copies[i, j, k].wait_recv()
    for copy in copies.values():
        copy.wait_send()


def gather_kernel(sizes, moved, mass, out, part, got_z, got, send_z, recv_z, send_sem, recv_sem):
    nx, ny, nz = sizes
    own = tuple(own_kind(n) for n in sizes)

    def place(i, j, k):
        return (i * kinds(ny) + j) * kinds(nz) + k

    greet(sizes)
    copies = []

    def send(src, dst, send_at, recv_at, device):
        copy = pltpu.make_async_remote_copy(
            src_ref=src, dst_ref=dst, send_sem=send_at, recv_sem=recv_at, device_id=device, device_id_type=MESH
        )
        copy.start()
        copies.append(copy)
        return copy

    columns = columns_of(sizes)
    order = [at for at, _ in columns] + [own[:2]]
    along_z, arriving = {}, {}
    for i, j in order:
        for k, device in cores_of(sizes):
            at = place(i, j, k)
            along_z[i, j, k] = send(moved.at[at], got_z.at[at], send_z.at[at], recv_z.at[at], device)

    def send_part(index):
        (i, j), device = columns[index]
        at = i * kinds(ny) + j
        arriving[at] = send(part.at[at], got.at[at], send_sem.at[at], recv_sem.at[at], device)

    for index, (i, j) in enumerate(order):
        total = moved[place(i, j, own[2])]
        for k, _ in steps_of(nz):
            along_z[i, j, k].wait_recv()
            total = total + got_z[place(i, j, k)]
        if index < len(columns):
            part[i * kinds(ny) + j] = total
        if index:
            send_part(index - 1)
    for at in reversed(list(arriving)):
        arriving[at].wait_recv()
        total = total + got[at]
    out[...] = total / mass[...]
    for copy in copies:
        copy.wait_send()


def split3(value):
    first = value.astype(jnp.bfloat16).astype(jnp.float32)
    rest = value - first
    second = rest.astype(jnp.bfloat16).astype(jnp.float32)
    return first, second, rest - second


def offsets():
    return [(a, b, c) for a in (-1, 0, 1) for b in (-1, 0, 1) for c in (-1, 0, 1)]


def kind_at(offset, count):
    if count >= 3:
        return offset + 1
    return abs(offset) if count == 2 else 0


def place_at(offset, sizes):
    i, j, k = (kind_at(o, n) for o, n in zip(offset, sizes))
    return (i * kinds(sizes[1]) + j) * kinds(sizes[2]) + k


PARTS = 16


def gas_features(gas, feat, slot, offset, tiles):
    px, py, pz = (gas[k] + (offset[k] - 0.5) for k in range(3))
    root = lax.rsqrt(gas[3])
    square = (px * px + py * py + pz * pz) * root
    rows = [split3(v) for v in (px * root, py * root, pz * root, square, root)]
    base = slot * tiles * PARTS
    for part in range(3):
        for comp in range(5):
            feat[pl.ds(base + part * 5 + comp, tiles, stride=PARTS), :] = rows[comp][part]
    feat[pl.ds(base + 15, tiles, stride=PARTS), :] = jnp.zeros_like(px)


def source_features(pos, radius, yields, momentum, rows, left, loads):
    blocks = pos.shape[1]
    r = radius[...]
    inv = 1.0 / (r * r)
    sx, sy, sz = (pos[k] - 0.5 for k in range(3))
    comps = [-2.0 * inv * sx, -2.0 * inv * sy, -2.0 * inv * sz, inv, 1.0 + inv * (sx * sx + sy * sy + sz * sz)]
    parts = [split3(v) for v in comps]
    zero = jnp.zeros_like(r)
    for group in range(3):
        for part in range(3):
            for comp in range(5):
                value = parts[comp][group] if part + group < 3 else zero
                rows[pl.ds(group * PARTS + part * 5 + comp, blocks, stride=3 * PARTS), :] = value
        rows[pl.ds(group * PARTS + 15, blocks, stride=3 * PARTS), :] = zero
    for b in range(blocks):
        left[b] = rows[b * 3 * PARTS : (b + 1) * 3 * PARTS, :].T.astype(jnp.bfloat16)
    for q, value in enumerate([yields[0], momentum[0], momentum[1], momentum[2], yields[1], zero, zero, zero]):
        loads[pl.ds(q, blocks, stride=8), :] = value


def one_block(b, table, count, feat, left, loads, moved):
    listed = table.shape[0]
    lhs = left[b]
    norm_acc = jnp.zeros((128, 128), jnp.float32)
    weights = []

    def tile_of(j):
        at = pl.multiple_of(table[j, b] * PARTS, PARTS)
        return feat[pl.ds(at, PARTS), :].astype(jnp.bfloat16)

    for j in range(0, listed, 2):
        rhs = jnp.concatenate([tile_of(j), tile_of(j + 1)], axis=1)
        u = jnp.dot(lhs, jnp.concatenate([rhs] * 3, axis=0), preferred_element_type=jnp.float32)
        w = 1.0 / (u * u)
        norm_acc = norm_acc + (w[:, :128] + w[:, 128:])
        w1 = w.astype(jnp.bfloat16)
        weights.append((w1, (w - w1.astype(jnp.float32)).astype(jnp.bfloat16)))
    norm = jnp.sum(norm_acc.T, axis=0, keepdims=True)
    lane = lax.broadcasted_iota(jnp.int32, (1, 128), 1)
    live = jnp.where(b * 128 + lane < count[0], 1.0, 0.0)
    coef = loads[pl.ds(pl.multiple_of(b * 8, 8), 8), :] * (live / norm)
    c1 = coef.astype(jnp.bfloat16).astype(jnp.float32)
    c2 = coef - c1
    half = jnp.concatenate([c1, c2], axis=0).astype(jnp.bfloat16)
    lhs2 = jnp.concatenate([half, half], axis=1)
    for j in range(0, listed, 2):
        got = jnp.dot(lhs2, jnp.concatenate(weights[j // 2], axis=0), preferred_element_type=jnp.float32)
        both = got[0:8] + got[8:16]
        start = pl.multiple_of((b * listed + j) * 8, 16)
        moved[pl.ds(start, 8), :] = both[:, :128]
        moved[pl.ds(start + 8, 8), :] = both[:, 128:]


def scatter(sizes, table_rows, moved, out):
    listed, blocks = table_rows.shape
    slots, _, tiles, _ = out.shape
    ids = table_rows[...]
    slot, tile = ids // tiles, ids % tiles
    nx, ny, nz = sizes
    at = kind_of(slot // 9 - 1, nx) * kinds(ny) + kind_of(slot // 3 % 3 - 1, ny)
    at = (at * kinds(nz) + kind_of(slot % 3 - 1, nz)) * tiles + tile
    rows = slots * tiles
    target = lax.broadcasted_iota(jnp.int32, (rows, listed), 0)
    ones = []
    for b in range(blocks):
        ones.append(at[:, b : b + 1])
    column = jnp.concatenate(ones, axis=0)
    pairs = blocks * listed
    hot = (column == lax.broadcasted_iota(jnp.int32, (pairs, rows), 1)).astype(jnp.float32)
    hot = hot.T.astype(jnp.bfloat16)
    hot = jnp.concatenate([hot, hot], axis=1)
    for q in range(5):
        value = moved[pl.ds(q, pairs, stride=8), :]
        m1 = value.astype(jnp.bfloat16)
        m2 = (value - m1.astype(jnp.float32)).astype(jnp.bfloat16)
        got = jnp.dot(hot, jnp.concatenate([m1, m2], axis=0), preferred_element_type=jnp.float32)
        for s in range(slots):
            out[s, q] = got[s * tiles : (s + 1) * tiles]


def deposit_kernel(sizes, unroll, table, count, table_rows, near, pos, radius, yields, momentum, out, feat, rows, left, loads, moved):
    blocks, listed = pos.shape[1], table.shape[0]
    slots, _, tiles, _ = near.shape
    for slot, offset in enumerate(offsets()):
        gas = [near[place_at(offset, sizes), k] for k in range(4)]
        gas_features(gas, feat, slot, offset, tiles)
    source_features(pos, radius, yields, momentum, rows, left, loads)

    def step(i, carry):
        for k in range(unroll):
            one_block(i * unroll + k, table, count, feat, left, loads, moved)
        return carry

    lax.fori_loop(0, blocks // unroll, step, 0)
    scatter(sizes, table_rows, moved, out)


def local(sizes, gas_pos, gas_mass, source_pos, source_radius, source_yield, source_momentum, source_tiles, source_count):
    gas_size = gas_pos.shape[-1]
    tiles = gas_size // 128
    blocks = source_pos.shape[-1] // 128
    listed = source_tiles.shape[-1]
    nx, ny, nz = sizes
    slots = kinds(nx) * kinds(ny) * kinds(nz)
    vmem = pl.BlockSpec(memory_space=pltpu.VMEM)
    near = pl.pallas_call(
        functools.partial(spread_kernel, sizes),
        out_shape=pltpu.VMEM((slots, 4, tiles, 128), jnp.float32),
        in_specs=[vmem, vmem],
        out_specs=vmem,
        scratch_shapes=[
            pltpu.SemaphoreType.DMA((2,)),
            pltpu.SemaphoreType.DMA((slots,)),
            pltpu.SemaphoreType.DMA((slots,)),
        ],
        compiler_params=pltpu.CompilerParams(collective_id=0, has_side_effects=True, vmem_limit_bytes=LIMIT),
    )(gas_pos.reshape(3, tiles, 128), gas_mass.reshape(1, tiles, 128))
    unroll = math.gcd(blocks, 2)
    smem = pl.BlockSpec(memory_space=pltpu.SMEM)
    table = source_tiles.reshape(blocks, listed).T
    moved = pl.pallas_call(
        functools.partial(deposit_kernel, sizes, unroll),
        out_shape=pltpu.VMEM((slots, 5, tiles, 128), jnp.float32),
        in_specs=[smem, smem] + [vmem] * 6,
        out_specs=vmem,
        scratch_shapes=[
            pltpu.VMEM((27 * tiles * PARTS, 128), jnp.float32),
            pltpu.VMEM((blocks * 3 * PARTS, 128), jnp.float32),
            pltpu.VMEM((blocks, 128, 3 * PARTS), jnp.bfloat16),
            pltpu.VMEM((blocks * 8, 128), jnp.float32),
            pltpu.VMEM((blocks * listed * 8, 128), jnp.float32),
        ],
        compiler_params=pltpu.CompilerParams(vmem_limit_bytes=LIMIT),
    )(
        table,
        source_count.reshape(1),
        table,
        near,
        source_pos.reshape(3, blocks, 128),
        source_radius.reshape(blocks, 128),
        source_yield.reshape(2, blocks, 128),
        source_momentum.reshape(3, blocks, 128),
    )
    piece = (5, tiles, 128)
    sides = kinds(nx) * kinds(ny)
    gain = pl.pallas_call(
        functools.partial(gather_kernel, sizes),
        out_shape=jax.ShapeDtypeStruct(piece, jnp.float32),
        in_specs=[vmem, vmem],
        out_specs=vmem,
        scratch_shapes=[
            pltpu.VMEM((sides, *piece), jnp.float32),
            pltpu.VMEM((slots, *piece), jnp.float32),
            pltpu.VMEM((sides, *piece), jnp.float32),
            pltpu.SemaphoreType.DMA((slots,)),
            pltpu.SemaphoreType.DMA((slots,)),
            pltpu.SemaphoreType.DMA((sides,)),
            pltpu.SemaphoreType.DMA((sides,)),
        ],
        compiler_params=pltpu.CompilerParams(collective_id=1, has_side_effects=True, vmem_limit_bytes=LIMIT),
    )(moved, gas_mass.reshape(1, tiles, 128))
    return gain.reshape(5, 1, 1, 1, gas_size)


def solution(mesh):
    sizes = (mesh.shape["gx"], mesh.shape["gy"], mesh.shape["gz"])
    in_specs = (
        P(None, "gx", "gy", "gz", None),
        P("gx", "gy", "gz", None),
        P(None, "gx", "gy", "gz", None),
        P("gx", "gy", "gz", None),
        P(None, "gx", "gy", "gz", None),
        P(None, "gx", "gy", "gz", None),
        P("gx", "gy", "gz", None, None),
        P("gx", "gy", "gz"),
    )
    out_specs = P(None, "gx", "gy", "gz", None)
    return jax.shard_map(
        functools.partial(local, sizes), mesh=mesh, in_specs=in_specs, out_specs=out_specs, check_vma=False
    )
```

```python
import functools
import math

import jax
import jax.numpy as jnp
from jax import lax
from jax.experimental import pallas as pl
from jax.experimental.pallas import tpu as pltpu
from jax.sharding import PartitionSpec as P


def kinds(count):
    return min(count, 3)


def kind_of(offset, count):
    if count >= 3:
        return offset + 1
    if count == 2:
        return jnp.abs(offset)
    return offset * 0


def own_kind(count):
    return 1 if count >= 3 else 0


def steps_of(count):
    if count >= 3:
        return ((0, -1), (2, 1))
    return ((1, 1),) if count == 2 else ()


MESH = pl.DeviceIdType.MESH
LIMIT = 48 * 1024 * 1024


def shifted(axis, count, step):
    return lax.rem(lax.axis_index(axis) + step + count, count)


def columns_of(sizes):
    nx, ny, _ = sizes
    choices_x = steps_of(nx) + ((own_kind(nx), 0),)
    choices_y = ((own_kind(ny), 0),) + steps_of(ny)
    return [
        ((i, j), {"gx": shifted("gx", nx, dx), "gy": shifted("gy", ny, dy)})
        for i, dx in choices_x
        for j, dy in choices_y
        if dx or dy
    ]


def cores_of(sizes):
    return [(k, {"gz": shifted("gz", sizes[2], dz)}) for k, dz in steps_of(sizes[2])]


def greet(sizes):
    barrier = pltpu.get_barrier_semaphore()
    peers = columns_of(sizes) + cores_of(sizes)
    for _, device in peers:
        pl.semaphore_signal(barrier, inc=1, device_id=device, device_id_type=MESH)
    if peers:
        pl.semaphore_wait(barrier, len(peers))


def facing(kind, count):
    return 2 - kind if count >= 3 else kind


PARTS = 16


def split3(value):
    first = value.astype(jnp.bfloat16).astype(jnp.float32)
    rest = value - first
    second = rest.astype(jnp.bfloat16).astype(jnp.float32)
    return first, second, rest - second


def offsets():
    return [(a, b, c) for a in (-1, 0, 1) for b in (-1, 0, 1) for c in (-1, 0, 1)]


def kind_at(offset, count):
    if count >= 3:
        return offset + 1
    return abs(offset) if count == 2 else 0


def place_at(offset, sizes):
    i, j, k = (kind_at(o, n) for o, n in zip(offset, sizes))
    return (i * kinds(sizes[1]) + j) * kinds(sizes[2]) + k


def role_places(role, sizes):
    places = [place_at(o, sizes) for o in offsets() if (o[0] != 0, o[1] != 0) == (role >= 2, role % 2 == 1)]
    return sorted(set(places))


def role_slots(role):
    return [n for n, o in enumerate(offsets()) if (o[0] != 0, o[1] != 0) == (role >= 2, role % 2 == 1)]


def gas_features(gas, feat, slot, offset):
    tiles = gas[3].shape[0]
    px, py, pz = (gas[k] + (offset[k] - 0.5) for k in range(3))
    root = lax.rsqrt(gas[3])
    square = (px * px + py * py + pz * pz) * root
    base = [n for role in range(4) for n in role_slots(role)].index(slot) * tiles
    for comp, value in enumerate((px * root, py * root, pz * root, square, root)):
        for part, piece in enumerate(split3(value)):
            at = (part * 5 + comp) * 128
            feat[base : base + tiles, at : at + 128] = piece.astype(jnp.bfloat16)


def source_features(pos, radius, rows, left):
    blocks = pos.shape[1]
    r = radius[...]
    inv = 1.0 / (r * r)
    sx, sy, sz = (pos[k] - 0.5 for k in range(3))
    comps = [-2.0 * inv * sx, -2.0 * inv * sy, -2.0 * inv * sz, inv, 1.0 + inv * (sx * sx + sy * sy + sz * sz)]
    parts = [split3(v) for v in comps]
    zero = jnp.zeros_like(r)
    for group in range(3):
        for part in range(3):
            for comp in range(5):
                value = parts[comp][group] if part + group < 3 else zero
                rows[pl.ds(group * PARTS + part * 5 + comp, blocks, stride=3 * PARTS), :] = value
        rows[pl.ds(group * PARTS + 15, blocks, stride=3 * PARTS), :] = zero
    for b in range(blocks):
        left[b] = rows[b * 3 * PARTS : (b + 1) * 3 * PARTS, :].T.astype(jnp.bfloat16)


def over_blocks(blocks, unroll, body):
    def step(i, carry):
        for k in range(unroll):
            body(i * unroll + k)
        return carry

    lax.fori_loop(0, blocks // unroll, step, 0)


def gather(role, tiles, feat, hot_in, picked):
    slots = [n for r in range(4) for n in role_slots(r)]
    first = slots.index(role_slots(role)[0]) * tiles
    depth = len(role_slots(role)) * tiles
    pairs = hot_in.shape[1]
    got = jnp.dot(hot_in[role, :, 0:depth], feat[first : first + depth, :], preferred_element_type=jnp.float32)
    for row in range(PARTS - 1):
        picked[role % 2, pl.ds(row, pairs, stride=PARTS), :] = got[:, row * 128 : row * 128 + 128]


def weigh(role, picked, left, weights, sums, norms, unroll):
    blocks = left.shape[0]

    def body(b):
        near = []
        for z in range(2):
            at = pl.multiple_of((z * blocks + b) * PARTS, PARTS)
            near.append(picked[role % 2, pl.ds(at, PARTS), :].astype(jnp.bfloat16))
        rhs = jnp.concatenate([jnp.concatenate(near, axis=1)] * 3, axis=0)
        u = jnp.dot(left[b], rhs, preferred_element_type=jnp.float32)
        w = 1.0 / (u * u)
        part = w[:, :128] + w[:, 128:]
        if role:
            part = sums[b] + part
        if role < 3:
            sums[b] = part
        else:
            norms[pl.ds(b, 1), :] = jnp.sum(part.T, axis=0, keepdims=True)
        w1 = w.astype(jnp.bfloat16)
        weights[role, b, 0:128] = w1
        weights[role, b, 128:256] = (w - w1.astype(jnp.float32)).astype(jnp.bfloat16)

    over_blocks(blocks, unroll, body)


def normalise(count, norms, yields, momentum, loads):
    blocks = norms.shape[0]
    lane = lax.broadcasted_iota(jnp.int32, (blocks, 128), 1)
    index = lax.broadcasted_iota(jnp.int32, (blocks, 128), 0) * 128 + lane
    scale = jnp.where(index < count[0], 1.0, 0.0) / norms[...]
    zero = jnp.zeros_like(scale)
    for q, value in enumerate([yields[0], momentum[0], momentum[1], momentum[2], yields[1], zero, zero, zero]):
        coef = value * scale
        high = coef.astype(jnp.bfloat16).astype(jnp.float32)
        loads[pl.ds(q, blocks, stride=16), :] = high
        loads[pl.ds(q + 8, blocks, stride=16), :] = coef - high


def deposit(role, loads, weights, moved, unroll):
    blocks = weights.shape[1]

    def body(b):
        half = loads[pl.ds(pl.multiple_of(b * 16, 16), 16), :].astype(jnp.bfloat16)
        got = jnp.dot(jnp.concatenate([half, half], axis=1), weights[role, b], preferred_element_type=jnp.float32)
        both = got[0:8] + got[8:16]
        for z in range(2):
            start = pl.multiple_of((z * blocks + b) * 8, 8)
            moved[role, pl.ds(start, 8), :] = both[:, z * 128 : z * 128 + 128]

    over_blocks(blocks, unroll, body)


def one_hots(sizes, tiles, table_rows, hot_in, hot_out):
    nx, ny, nz = sizes
    ids = table_rows[...]
    slot, tile = ids // tiles, ids % tiles
    at = kind_of(slot // 9 - 1, nx) * kinds(ny) + kind_of(slot // 3 % 3 - 1, ny)
    at = (at * kinds(nz) + kind_of(slot % 3 - 1, nz)) * tiles + tile
    flip_a = slot[0:1] // 9 == 0
    flip_b = slot[0:1] // 3 % 3 == 0

    def pick(values, role):
        row = []
        for z in range(2):
            low, high = (
                jnp.where(flip_b, values[4 * a + z + 2 : 4 * a + z + 3], values[4 * a + z : 4 * a + z + 1])
                if role % 2 == 0
                else jnp.where(flip_b, values[4 * a + z : 4 * a + z + 1], values[4 * a + z + 2 : 4 * a + z + 3])
                for a in range(2)
            )
            row.append(jnp.where(flip_a, high, low) if role < 2 else jnp.where(flip_a, low, high))
        return jnp.concatenate(row, axis=1)

    for role in range(4):
        source, target = pick(ids, role), pick(at, role)
        pairs = source.shape[1]
        index = lax.broadcasted_iota(jnp.int32, (tiles, pairs), 0)
        hot = [(index + n * tiles == source).astype(jnp.float32) for n in role_slots(role)]
        depth = len(hot) * tiles
        hot_in[role, :, 0:depth] = jnp.concatenate(hot, axis=0).T.astype(jnp.bfloat16)
        hot = [(index + n * tiles == target).astype(jnp.float32) for n in role_places(role, sizes)]
        hot = jnp.concatenate(hot, axis=0).astype(jnp.bfloat16)
        hot_out[role, 0 : hot.shape[0], :] = jnp.concatenate([hot, hot], axis=1)


def scatter(role, sizes, hot_out, moved, out, done):
    tiles = out.shape[2]
    places = role_places(role, sizes)
    pairs = hot_out.shape[2] // 2
    values = jnp.concatenate([moved[role, pl.ds(q, pairs, stride=8), :] for q in range(5)], axis=1)
    m1 = values.astype(jnp.bfloat16)
    m2 = (values - m1.astype(jnp.float32)).astype(jnp.bfloat16)
    hot = hot_out[role, 0 : len(places) * tiles, :]
    got = jnp.dot(hot, jnp.concatenate([m1, m2], axis=0), preferred_element_type=jnp.float32)
    for n, place in enumerate(places):
        for q in range(5):
            value = got[n * tiles : (n + 1) * tiles, q * 128 : (q + 1) * 128]
            out[place, q] = out[place, q] + value if place in done else value
        done.add(place)


def core_scratch(blocks, tiles):
    return [
        pltpu.VMEM((27 * tiles, (PARTS - 1) * 128), jnp.bfloat16),
        pltpu.VMEM((blocks * 3 * PARTS, 128), jnp.float32),
        pltpu.VMEM((blocks, 128, 3 * PARTS), jnp.bfloat16),
        pltpu.VMEM((4, blocks, 256, 256), jnp.bfloat16),
        pltpu.VMEM((blocks, 128, 128), jnp.float32),
        pltpu.VMEM((blocks, 128), jnp.float32),
        pltpu.VMEM((blocks * 16, 128), jnp.float32),
        pltpu.VMEM((4, blocks * 16, 128), jnp.float32),
        pltpu.VMEM((4, 2 * blocks, 12 * tiles), jnp.bfloat16),
        pltpu.VMEM((4, 12 * tiles, 4 * blocks), jnp.bfloat16),
        pltpu.VMEM((2, 2 * blocks * PARTS, 128), jnp.float32),
    ]


def fused_kernel(sizes, pos, mass, table, count, spos, sradius, syield, smomentum, out, *scratch):
    (near, count_s, table_v, pos_v, radius_v, yield_v, momentum_v, deposits, part, got_z, got) = scratch[:11]
    (feat, rows, left, weights, sums, norms, loads, moved, hot_in, hot_out, picked) = scratch[11:22]
    local_sem, send_sem, recv_sem, gsend_z, grecv_z, gsend, grecv = scratch[22:]
    nx, ny, nz = sizes
    own = tuple(own_kind(n) for n in sizes)
    tiles = near.shape[2]
    blocks = pos_v.shape[1]
    unroll = math.gcd(blocks, 16)

    def place(i, j, k):
        return (i * kinds(ny) + j) * kinds(nz) + k

    home = place(*own)
    gas_in = [
        pltpu.make_async_copy(pos, near.at[home, pl.ds(0, 3)], local_sem.at[0]),
        pltpu.make_async_copy(mass, near.at[home, pl.ds(3, 1)], local_sem.at[1]),
    ]
    pairs = [(spos, pos_v), (sradius, radius_v), (syield, yield_v), (smomentum, momentum_v)]
    pairs += [(count, count_s), (table, table_v)]
    rest_in = [pltpu.make_async_copy(src, dst, local_sem.at[2 + n]) for n, (src, dst) in enumerate(pairs)]
    for copy in gas_in + rest_in:
        copy.start()
    greet(sizes)
    for copy in gas_in:
        copy.wait()
    copies = {}
    finished = []

    def send(slot, there, device):
        target = place(*there)
        copy = pltpu.make_async_remote_copy(
            src_ref=near.at[place(*slot)],
            dst_ref=near.at[target],
            send_sem=send_sem.at[target],
            recv_sem=recv_sem.at[target],
            device_id=device,
            device_id_type=MESH,
        )
        copy.start()
        copies[there] = copy
        finished.append(copy)

    def to_cores(i, j):
        for k, device in cores_of(sizes):
            send((i, j, own[2]), (i, j, facing(k, nz)), device)

    columns = columns_of(sizes)
    for (i, j), device in columns:
        send(own, (facing(i, nx), facing(j, ny), own[2]), device)
    to_cores(own[0], own[1])
    for copy in rest_in:
        copy.wait()

    def features(i, j, k):
        for slot, offset in enumerate(offsets()):
            if place_at(offset, sizes) == place(i, j, k):
                gas_features([near[place(i, j, k), c] for c in range(4)], feat, slot, offset)

    def weigh_role(role):
        gather(role, tiles, feat, hot_in, picked)
        weigh(role, picked, left, weights, sums, norms, unroll)

    source_features(pos_v, radius_v, rows, left)
    one_hots(sizes, tiles, table_v, hot_in, hot_out)
    spare = jnp.zeros((2 * blocks, 128), jnp.float32)
    for side in range(2):
        picked[side, pl.ds(PARTS - 1, 2 * blocks, stride=PARTS), :] = spare
    features(*own)
    for k, _ in steps_of(nz):
        copies[own[0], own[1], k].wait_recv()
        features(own[0], own[1], k)
    weigh_role(0)
    across = [at for at, _ in columns if at[0] != own[0]]
    along = [at for at, _ in columns if at[0] == own[0]]
    for at in along + across:
        copies[at[0], at[1], own[2]].wait_recv()
        to_cores(*at)
        features(at[0], at[1], own[2])
    for role in (1, 2, 3):
        for i, j in along + across:
            if (i != own[0], j != own[1]) == (role >= 2, role % 2 == 1):
                for k, _ in steps_of(nz):
                    copies[i, j, k].wait_recv()
                    features(i, j, k)
        weigh_role(role)
    normalise(count_s, norms, yield_v, momentum_v, loads)
    done = set()
    along_z, arriving = {}, {}

    def send_gain(src, dst, send_at, recv_at, device):
        copy = pltpu.make_async_remote_copy(
            src_ref=src, dst_ref=dst, send_sem=send_at, recv_sem=recv_at, device_id=device, device_id_type=MESH
        )
        copy.start()
        finished.append(copy)
        return copy

    def role_of(at):
        return 2 * (at[0] != own[0]) + (at[1] != own[1])

    def send_z(i, j):
        for k, device in cores_of(sizes):
            at = place(i, j, k)
            along_z[i, j, k] = send_gain(deposits.at[at], got_z.at[at], gsend_z.at[at], grecv_z.at[at], device)

    for role in (3, 2, 1, 0):
        deposit(role, loads, weights, moved, unroll)
        scatter(role, sizes, hot_out, moved, deposits, done)
        for i, j in [at for at, _ in columns] + [own[:2]]:
            if role_of((i, j)) == role:
                send_z(i, j)
    ordered = sorted(columns, key=lambda c: -role_of(c[0]))

    def send_part(index):
        (i, j), device = ordered[index]
        at = i * kinds(ny) + j
        arriving[at] = send_gain(part.at[at], got.at[at], gsend.at[at], grecv.at[at], device)

    order = [at for at, _ in ordered] + [own[:2]]
    for index, (i, j) in enumerate(order):
        total = deposits[place(i, j, own[2])]
        for k, _ in steps_of(nz):
            along_z[i, j, k].wait_recv()
            total = total + got_z[place(i, j, k)]
        if index < len(ordered):
            part[i * kinds(ny) + j] = total
        if index:
            send_part(index - 1)
    for at in reversed(list(arriving)):
        arriving[at].wait_recv()
        total = total + got[at]
    out[...] = total / near[home, 3]
    for copy in finished:
        copy.wait_send()


def local(sizes, gas_pos, gas_mass, source_pos, source_radius, source_yield, source_momentum, source_tiles, source_count):
    gas_size = gas_pos.shape[-1]
    tiles = gas_size // 128
    blocks = source_pos.shape[-1] // 128
    listed = source_tiles.shape[-1]
    slots = kinds(sizes[0]) * kinds(sizes[1]) * kinds(sizes[2])
    sides = kinds(sizes[0]) * kinds(sizes[1])
    piece = (5, tiles, 128)
    given = pl.BlockSpec(memory_space=pl.ANY)
    dma = pltpu.SemaphoreType.DMA
    gain = pl.pallas_call(
        functools.partial(fused_kernel, sizes),
        out_shape=jax.ShapeDtypeStruct(piece, jnp.float32),
        in_specs=[given] * 8,
        out_specs=pl.BlockSpec(memory_space=pltpu.VMEM),
        scratch_shapes=[
            pltpu.VMEM((slots, 4, tiles, 128), jnp.float32),
            pltpu.SMEM((1,), jnp.int32),
            pltpu.VMEM((listed, blocks), jnp.int32),
            pltpu.VMEM((3, blocks, 128), jnp.float32),
            pltpu.VMEM((blocks, 128), jnp.float32),
            pltpu.VMEM((2, blocks, 128), jnp.float32),
            pltpu.VMEM((3, blocks, 128), jnp.float32),
            pltpu.VMEM((slots, *piece), jnp.float32),
            pltpu.VMEM((sides, *piece), jnp.float32),
            pltpu.VMEM((slots, *piece), jnp.float32),
            pltpu.VMEM((sides, *piece), jnp.float32),
            *core_scratch(blocks, tiles),
            dma((8,)),
            dma((slots,)),
            dma((slots,)),
            dma((slots,)),
            dma((slots,)),
            dma((sides,)),
            dma((sides,)),
        ],
        compiler_params=pltpu.CompilerParams(collective_id=0, has_side_effects=True, vmem_limit_bytes=LIMIT),
    )(
        gas_pos.reshape(3, tiles, 128),
        gas_mass.reshape(1, tiles, 128),
        source_tiles.reshape(blocks, listed).T,
        source_count.reshape(1),
        source_pos.reshape(3, blocks, 128),
        source_radius.reshape(blocks, 128),
        source_yield.reshape(2, blocks, 128),
        source_momentum.reshape(3, blocks, 128),
    )
    return gain.reshape(5, 1, 1, 1, gas_size)


def solution(mesh):
    sizes = (mesh.shape["gx"], mesh.shape["gy"], mesh.shape["gz"])
    in_specs = (
        P(None, "gx", "gy", "gz", None),
        P("gx", "gy", "gz", None),
        P(None, "gx", "gy", "gz", None),
        P("gx", "gy", "gz", None),
        P(None, "gx", "gy", "gz", None),
        P(None, "gx", "gy", "gz", None),
        P("gx", "gy", "gz", None, None),
        P("gx", "gy", "gz"),
    )
    out_specs = P(None, "gx", "gy", "gz", None)
    return jax.shard_map(
        functools.partial(local, sizes), mesh=mesh, in_specs=in_specs, out_specs=out_specs, check_vma=False
    )
```

```python
import functools
import math

import jax
import jax.numpy as jnp
from jax import lax
from jax.experimental import pallas as pl
from jax.experimental.pallas import tpu as pltpu
from jax.sharding import PartitionSpec as P


def kinds(count):
    return min(count, 3)


def kind_of(offset, count):
    if count >= 3:
        return offset + 1
    if count == 2:
        return jnp.abs(offset)
    return offset * 0


def own_kind(count):
    return 1 if count >= 3 else 0


def steps_of(count):
    if count >= 3:
        return ((0, -1), (2, 1))
    return ((1, 1),) if count == 2 else ()


MESH = pl.DeviceIdType.MESH
LIMIT = 67_043_328 - 64 * 1024


def shifted(axis, count, step):
    return lax.rem(lax.axis_index(axis) + step + count, count)


def columns_of(sizes):
    nx, ny, _ = sizes
    choices_x = steps_of(nx) + ((own_kind(nx), 0),)
    choices_y = ((own_kind(ny), 0),) + steps_of(ny)
    return [
        ((i, j), {"gx": shifted("gx", nx, dx), "gy": shifted("gy", ny, dy)})
        for i, dx in choices_x
        for j, dy in choices_y
        if dx or dy
    ]


def cores_of(sizes):
    return [(k, {"gz": shifted("gz", sizes[2], dz)}) for k, dz in steps_of(sizes[2])]


def greet(sizes):
    barrier = pltpu.get_barrier_semaphore()
    peers = columns_of(sizes) + cores_of(sizes)
    for _, device in peers:
        pl.semaphore_signal(barrier, inc=1, device_id=device, device_id_type=MESH)
    if peers:
        pl.semaphore_wait(barrier, len(peers))


def facing(kind, count):
    return 2 - kind if count >= 3 else kind


PARTS = 16


def split3(value):
    first = value.astype(jnp.bfloat16).astype(jnp.float32)
    rest = value - first
    second = rest.astype(jnp.bfloat16).astype(jnp.float32)
    return first, second, rest - second


def offsets():
    return [(a, b, c) for a in (-1, 0, 1) for b in (-1, 0, 1) for c in (-1, 0, 1)]


def kind_at(offset, count):
    if count >= 3:
        return offset + 1
    return abs(offset) if count == 2 else 0


def place_at(offset, sizes):
    i, j, k = (kind_at(o, n) for o, n in zip(offset, sizes))
    return (i * kinds(sizes[1]) + j) * kinds(sizes[2]) + k


def role_places(role, sizes):
    places = [place_at(o, sizes) for o in offsets() if (o[0] != 0, o[1] != 0) == (role >= 2, role % 2 == 1)]
    return sorted(set(places))


def role_slots(role):
    return [n for n, o in enumerate(offsets()) if (o[0] != 0, o[1] != 0) == (role >= 2, role % 2 == 1)]


def gas_features(gas, feat, slot, offset):
    tiles = gas[3].shape[0]
    px, py, pz = (gas[k] + (offset[k] - 0.5) for k in range(3))
    root = lax.rsqrt(gas[3])
    square = (px * px + py * py + pz * pz) * root
    base = [n for role in range(4) for n in role_slots(role)].index(slot) * tiles
    for comp, value in enumerate((px * root, py * root, pz * root, square, root)):
        for part, piece in enumerate(split3(value)):
            at = (part * 5 + comp) * 128
            feat[base : base + tiles, at : at + 128] = piece.astype(jnp.bfloat16)


def source_features(pos, radius, rows, left):
    blocks = pos.shape[1]
    r = radius[...]
    inv = 1.0 / (r * r)
    sx, sy, sz = (pos[k] - 0.5 for k in range(3))
    comps = [-2.0 * inv * sx, -2.0 * inv * sy, -2.0 * inv * sz, inv, 1.0 + inv * (sx * sx + sy * sy + sz * sz)]
    parts = [split3(v) for v in comps]
    zero = jnp.zeros_like(r)
    for group in range(3):
        for part in range(3):
            for comp in range(5):
                value = parts[comp][group] if part + group < 3 else zero
                rows[pl.ds(group * PARTS + part * 5 + comp, blocks, stride=3 * PARTS), :] = value
        rows[pl.ds(group * PARTS + 15, blocks, stride=3 * PARTS), :] = zero
    for b in range(blocks):
        left[b] = rows[b * 3 * PARTS : (b + 1) * 3 * PARTS, :].T.astype(jnp.bfloat16)


def over_blocks(blocks, unroll, body):
    def step(i, carry):
        for k in range(unroll):
            body(i * unroll + k)
        return carry

    lax.fori_loop(0, blocks // unroll, step, 0)


def gather(role, tiles, feat, hot_in, picked):
    slots = [n for r in range(4) for n in role_slots(r)]
    first = slots.index(role_slots(role)[0]) * tiles
    depth = len(role_slots(role)) * tiles
    pairs = hot_in.shape[1]
    got = jnp.dot(hot_in[role, :, 0:depth], feat[first : first + depth, :], preferred_element_type=jnp.float32)
    for row in range(PARTS - 1):
        picked[role % 2, pl.ds(row, pairs, stride=PARTS), :] = got[:, row * 128 : row * 128 + 128]


def weigh(role, picked, left, weights, sums, norms, unroll):
    blocks = left.shape[0]

    def body(b):
        near = []
        for z in range(2):
            at = pl.multiple_of((z * blocks + b) * PARTS, PARTS)
            near.append(picked[role % 2, pl.ds(at, PARTS), :].astype(jnp.bfloat16))
        rhs = jnp.concatenate([jnp.concatenate(near, axis=1)] * 3, axis=0)
        u = jnp.dot(left[b], rhs, preferred_element_type=jnp.float32)
        w = 1.0 / (u * u)
        part = w[:, :128] + w[:, 128:]
        if role:
            part = sums[b] + part
        if role < 3:
            sums[b] = part
        else:
            norms[pl.ds(b, 1), :] = jnp.sum(part.T, axis=0, keepdims=True)
        w1 = w.astype(jnp.bfloat16)
        weights[role, b, 0:128] = w1
        weights[role, b, 128:256] = (w - w1.astype(jnp.float32)).astype(jnp.bfloat16)

    over_blocks(blocks, unroll, body)


def normalise(count, norms, yields, momentum, loads):
    blocks = norms.shape[0]
    lane = lax.broadcasted_iota(jnp.int32, (blocks, 128), 1)
    index = lax.broadcasted_iota(jnp.int32, (blocks, 128), 0) * 128 + lane
    scale = jnp.where(index < count[0, 0], 1.0, 0.0) / norms[...]
    zero = jnp.zeros_like(scale)
    for q, value in enumerate([yields[0], momentum[0], momentum[1], momentum[2], yields[1], zero, zero, zero]):
        coef = value * scale
        high = coef.astype(jnp.bfloat16).astype(jnp.float32)
        loads[pl.ds(q, blocks, stride=16), :] = high
        loads[pl.ds(q + 8, blocks, stride=16), :] = coef - high


def deposit(role, loads, weights, moved, unroll):
    blocks = weights.shape[1]

    def body(b):
        half = loads[pl.ds(pl.multiple_of(b * 16, 16), 16), :].astype(jnp.bfloat16)
        got = jnp.dot(jnp.concatenate([half, half], axis=1), weights[role, b], preferred_element_type=jnp.float32)
        both = got[0:8] + got[8:16]
        for z in range(2):
            start = pl.multiple_of((z * blocks + b) * 8, 8)
            moved[role, pl.ds(start, 8), :] = both[:, z * 128 : z * 128 + 128]

    over_blocks(blocks, unroll, body)


def one_hots(sizes, tiles, table_rows, hot_in, hot_out):
    nx, ny, nz = sizes
    ids = table_rows[...]
    slot, tile = ids // tiles, ids % tiles
    at = kind_of(slot // 9 - 1, nx) * kinds(ny) + kind_of(slot // 3 % 3 - 1, ny)
    at = (at * kinds(nz) + kind_of(slot % 3 - 1, nz)) * tiles + tile
    flip_a = slot[0:1] // 9 == 0
    flip_b = slot[0:1] // 3 % 3 == 0

    def pick(values, role):
        row = []
        for z in range(2):
            low, high = (
                jnp.where(flip_b, values[4 * a + z + 2 : 4 * a + z + 3], values[4 * a + z : 4 * a + z + 1])
                if role % 2 == 0
                else jnp.where(flip_b, values[4 * a + z : 4 * a + z + 1], values[4 * a + z + 2 : 4 * a + z + 3])
                for a in range(2)
            )
            row.append(jnp.where(flip_a, high, low) if role < 2 else jnp.where(flip_a, low, high))
        return jnp.concatenate(row, axis=1)

    for role in range(4):
        source, target = pick(ids, role), pick(at, role)
        pairs = source.shape[1]
        index = lax.broadcasted_iota(jnp.int32, (tiles, pairs), 0)
        hot = [(index + n * tiles == source).astype(jnp.float32) for n in role_slots(role)]
        depth = len(hot) * tiles
        hot_in[role, :, 0:depth] = jnp.concatenate(hot, axis=0).T.astype(jnp.bfloat16)
        hot = [(index + n * tiles == target).astype(jnp.float32) for n in role_places(role, sizes)]
        hot = jnp.concatenate(hot, axis=0).astype(jnp.bfloat16)
        hot_out[role, 0 : hot.shape[0], :] = jnp.concatenate([hot, hot], axis=1)


def scatter(role, sizes, hot_out, moved, out, done):
    tiles = out.shape[2]
    places = role_places(role, sizes)
    pairs = hot_out.shape[2] // 2
    values = jnp.concatenate([moved[role, pl.ds(q, pairs, stride=8), :] for q in range(5)], axis=1)
    m1 = values.astype(jnp.bfloat16)
    m2 = (values - m1.astype(jnp.float32)).astype(jnp.bfloat16)
    hot = hot_out[role, 0 : len(places) * tiles, :]
    got = jnp.dot(hot, jnp.concatenate([m1, m2], axis=0), preferred_element_type=jnp.float32)
    for n, place in enumerate(places):
        for q in range(5):
            value = got[n * tiles : (n + 1) * tiles, q * 128 : (q + 1) * 128]
            out[place, q] = out[place, q] + value if place in done else value
        done.add(place)


def core_scratch(blocks, tiles):
    return [
        pltpu.VMEM((27 * tiles, (PARTS - 1) * 128), jnp.bfloat16),
        pltpu.VMEM((blocks * 3 * PARTS, 128), jnp.float32),
        pltpu.VMEM((blocks, 128, 3 * PARTS), jnp.bfloat16),
        pltpu.VMEM((4, blocks, 256, 256), jnp.bfloat16),
        pltpu.VMEM((blocks, 128, 128), jnp.float32),
        pltpu.VMEM((blocks, 128), jnp.float32),
        pltpu.VMEM((blocks * 16, 128), jnp.float32),
        pltpu.VMEM((4, blocks * 16, 128), jnp.float32),
        pltpu.VMEM((4, 2 * blocks, 12 * tiles), jnp.bfloat16),
        pltpu.VMEM((4, 12 * tiles, 4 * blocks), jnp.bfloat16),
        pltpu.VMEM((2, 2 * blocks * PARTS, 128), jnp.float32),
    ]


def fused_kernel(sizes, pos, mass, table, count, spos, sradius, syield, smomentum, out, *scratch):
    (near, count_s, table_v, pos_v, radius_v, yield_v, momentum_v, deposits, part, got_z, got) = scratch[:11]
    (feat, rows, left, weights, sums, norms, loads, moved, hot_in, hot_out, picked) = scratch[11:22]
    local_sem, send_sem, recv_sem, gsend_z, grecv_z, gsend, grecv = scratch[22:]
    nx, ny, nz = sizes
    own = tuple(own_kind(n) for n in sizes)
    tiles = near.shape[2]
    blocks = pos_v.shape[1]
    unroll = math.gcd(blocks, 16)

    def place(i, j, k):
        return (i * kinds(ny) + j) * kinds(nz) + k

    home = place(*own)
    gas_in = [
        pltpu.make_async_copy(pos, near.at[home, pl.ds(0, 3)], local_sem.at[0]),
        pltpu.make_async_copy(mass, near.at[home, pl.ds(3, 1)], local_sem.at[1]),
    ]
    pairs = [(spos, pos_v), (sradius, radius_v), (syield, yield_v), (smomentum, momentum_v)]
    pairs += [(count, count_s), (table, table_v)]
    rest_in = [pltpu.make_async_copy(src, dst, local_sem.at[2 + n]) for n, (src, dst) in enumerate(pairs)]
    for copy in gas_in + rest_in:
        copy.start()
    greet(sizes)
    for copy in gas_in:
        copy.wait()
    copies = {}
    finished = []

    def send(slot, there, device):
        target = place(*there)
        copy = pltpu.make_async_remote_copy(
            src_ref=near.at[place(*slot)],
            dst_ref=near.at[target],
            send_sem=send_sem.at[target],
            recv_sem=recv_sem.at[target],
            device_id=device,
            device_id_type=MESH,
        )
        copy.start()
        copies[there] = copy
        finished.append(copy)

    def to_cores(i, j):
        for k, device in cores_of(sizes):
            send((i, j, own[2]), (i, j, facing(k, nz)), device)

    columns = columns_of(sizes)
    for (i, j), device in columns:
        send(own, (facing(i, nx), facing(j, ny), own[2]), device)
    to_cores(own[0], own[1])
    for copy in rest_in:
        copy.wait()

    def features(i, j, k):
        for slot, offset in enumerate(offsets()):
            if place_at(offset, sizes) == place(i, j, k):
                gas_features([near[place(i, j, k), c] for c in range(4)], feat, slot, offset)

    def weigh_role(role):
        gather(role, tiles, feat, hot_in, picked)
        weigh(role, picked, left, weights, sums, norms, unroll)

    source_features(pos_v, radius_v, rows, left)
    one_hots(sizes, tiles, table_v, hot_in, hot_out)
    spare = jnp.zeros((2 * blocks, 128), jnp.float32)
    for side in range(2):
        picked[side, pl.ds(PARTS - 1, 2 * blocks, stride=PARTS), :] = spare
    features(*own)
    for k, _ in steps_of(nz):
        copies[own[0], own[1], k].wait_recv()
        features(own[0], own[1], k)
    weigh_role(0)
    across = [at for at, _ in columns if at[0] != own[0]]
    along = [at for at, _ in columns if at[0] == own[0]]
    for at in along + across:
        copies[at[0], at[1], own[2]].wait_recv()
        to_cores(*at)
        features(at[0], at[1], own[2])
    for role in (1, 2, 3):
        for i, j in along + across:
            if (i != own[0], j != own[1]) == (role >= 2, role % 2 == 1):
                for k, _ in steps_of(nz):
                    copies[i, j, k].wait_recv()
                    features(i, j, k)
        weigh_role(role)
    normalise(count_s, norms, yield_v, momentum_v, loads)
    done = set()
    along_z, arriving = {}, {}

    def send_gain(src, dst, send_at, recv_at, device):
        copy = pltpu.make_async_remote_copy(
            src_ref=src, dst_ref=dst, send_sem=send_at, recv_sem=recv_at, device_id=device, device_id_type=MESH
        )
        copy.start()
        finished.append(copy)
        return copy

    def role_of(at):
        return 2 * (at[0] != own[0]) + (at[1] != own[1])

    def send_z(i, j):
        for k, device in cores_of(sizes):
            at = place(i, j, k)
            along_z[i, j, k] = send_gain(deposits.at[at], got_z.at[at], gsend_z.at[at], grecv_z.at[at], device)

    for role in (3, 2, 1, 0):
        deposit(role, loads, weights, moved, unroll)
        scatter(role, sizes, hot_out, moved, deposits, done)
        for i, j in [at for at, _ in columns] + [own[:2]]:
            if role_of((i, j)) == role:
                send_z(i, j)
    ordered = sorted(columns, key=lambda c: -role_of(c[0]))

    def send_part(index):
        (i, j), device = ordered[index]
        at = i * kinds(ny) + j
        arriving[at] = send_gain(part.at[at], got.at[at], gsend.at[at], grecv.at[at], device)

    order = [at for at, _ in ordered] + [own[:2]]
    for index, (i, j) in enumerate(order):
        total = deposits[place(i, j, own[2])]
        for k, _ in steps_of(nz):
            along_z[i, j, k].wait_recv()
            total = total + got_z[place(i, j, k)]
        if index < len(ordered):
            part[i * kinds(ny) + j] = total
        if index:
            send_part(index - 1)
    for at in reversed(list(arriving)):
        arriving[at].wait_recv()
        total = total + got[at]
    out[...] = total / near[home, 3]
    for copy in finished:
        copy.wait_send()


def local(sizes, gas_pos, gas_mass, source_pos, source_radius, source_yield, source_momentum, source_tiles, source_count):
    gas_size = gas_pos.shape[-1]
    tiles = gas_size // 128
    blocks = source_pos.shape[-1] // 128
    listed = source_tiles.shape[-1]
    slots = kinds(sizes[0]) * kinds(sizes[1]) * kinds(sizes[2])
    sides = kinds(sizes[0]) * kinds(sizes[1])
    piece = (5, tiles, 128)
    given = pl.BlockSpec(memory_space=pltpu.HBM)
    dma = pltpu.SemaphoreType.DMA
    gain = pl.pallas_call(
        functools.partial(fused_kernel, sizes),
        out_shape=pltpu.VMEM(piece, jnp.float32),
        in_specs=[given] * 8,
        out_specs=pl.BlockSpec(memory_space=pltpu.VMEM),
        scratch_shapes=[
            pltpu.VMEM((slots, 4, tiles, 128), jnp.float32),
            pltpu.SMEM((1, 1), jnp.int32),
            pltpu.VMEM((listed, blocks), jnp.int32),
            pltpu.VMEM((3, blocks, 128), jnp.float32),
            pltpu.VMEM((blocks, 128), jnp.float32),
            pltpu.VMEM((2, blocks, 128), jnp.float32),
            pltpu.VMEM((3, blocks, 128), jnp.float32),
            pltpu.VMEM((slots, *piece), jnp.float32),
            pltpu.VMEM((sides, *piece), jnp.float32),
            pltpu.VMEM((slots, *piece), jnp.float32),
            pltpu.VMEM((sides, *piece), jnp.float32),
            *core_scratch(blocks, tiles),
            dma((8,)),
            dma((slots,)),
            dma((slots,)),
            dma((slots,)),
            dma((slots,)),
            dma((sides,)),
            dma((sides,)),
        ],
        compiler_params=pltpu.CompilerParams(collective_id=0, has_side_effects=True, vmem_limit_bytes=LIMIT),
    )(
        gas_pos.reshape(3, tiles, 128),
        gas_mass.reshape(1, tiles, 128),
        source_tiles.reshape(blocks, listed).T,
        source_count.reshape(1, 1),
        source_pos.reshape(3, blocks, 128),
        source_radius.reshape(blocks, 128),
        source_yield.reshape(2, blocks, 128),
        source_momentum.reshape(3, blocks, 128),
    )
    return gain.reshape(5, 1, 1, 1, gas_size)


def solution(mesh):
    sizes = (mesh.shape["gx"], mesh.shape["gy"], mesh.shape["gz"])
    in_specs = (
        P(None, "gx", "gy", "gz", None),
        P("gx", "gy", "gz", None),
        P(None, "gx", "gy", "gz", None),
        P("gx", "gy", "gz", None),
        P(None, "gx", "gy", "gz", None),
        P(None, "gx", "gy", "gz", None),
        P("gx", "gy", "gz", None, None),
        P("gx", "gy", "gz"),
    )
    out_specs = P(None, "gx", "gy", "gz", None)
    return jax.shard_map(
        functools.partial(local, sizes), mesh=mesh, in_specs=in_specs, out_specs=out_specs, check_vma=False
    )
```

```python
import functools
import math

import jax
import jax.numpy as jnp
from jax import lax
from jax.experimental import pallas as pl
from jax.experimental.pallas import tpu as pltpu
from jax.sharding import PartitionSpec as P


def kinds(count):
    return min(count, 3)


def kind_of(offset, count):
    if count >= 3:
        return offset + 1
    if count == 2:
        return jnp.abs(offset)
    return offset * 0


def own_kind(count):
    return 1 if count >= 3 else 0


def steps_of(count):
    if count >= 3:
        return ((0, -1), (2, 1))
    return ((1, 1),) if count == 2 else ()


MESH = pl.DeviceIdType.MESH
LIMIT = 67_043_328 - 64 * 1024


def shifted(axis, count, step):
    return lax.rem(lax.axis_index(axis) + step + count, count)


def columns_of(sizes):
    nx, ny, _ = sizes
    choices_x = steps_of(nx) + ((own_kind(nx), 0),)
    choices_y = ((own_kind(ny), 0),) + steps_of(ny)
    return [
        ((i, j), {"gx": shifted("gx", nx, dx), "gy": shifted("gy", ny, dy)})
        for i, dx in choices_x
        for j, dy in choices_y
        if dx or dy
    ]


def far_first(sizes):
    nx, ny, _ = sizes
    turn_x = 2 * lax.rem(lax.axis_index("gx"), 2) - 1
    turn_y = jnp.where(lax.axis_index("gy") == 0, -1, 1)
    choices_x = [(1 + turn_x, turn_x), (1 - turn_x, -turn_x)] if nx >= 3 else list(steps_of(nx))
    choices_y = [(1 + turn_y, turn_y), (1 - turn_y, -turn_y)] if ny >= 3 else list(steps_of(ny))
    own_x, own_y = (own_kind(nx), 0), (own_kind(ny), 0)
    order = [(x, y) for y in choices_y for x in choices_x + [own_x]] + [(x, own_y) for x in choices_x]
    return [((i, j), {"gx": shifted("gx", nx, dx), "gy": shifted("gy", ny, dy)}) for (i, dx), (j, dy) in order]


def far_roles(sizes):
    steps_x, steps_y = len(steps_of(sizes[0])), len(steps_of(sizes[1]))
    return ([3] * steps_x + [1]) * steps_y + [2] * steps_x


def facing_at(kind, count):
    return 2 - kind if count >= 3 else kind


def cores_of(sizes):
    return [(k, {"gz": shifted("gz", sizes[2], dz)}) for k, dz in steps_of(sizes[2])]


def greet(sizes, meanwhile):
    barrier = pltpu.get_barrier_semaphore()
    peers = columns_of(sizes) + cores_of(sizes)
    for _, device in peers:
        pl.semaphore_signal(barrier, inc=1, device_id=device, device_id_type=MESH)
    meanwhile()
    if peers:
        pl.semaphore_wait(barrier, len(peers))


def facing(kind, count):
    return 2 - kind if count >= 3 else kind


PARTS = 16


def split3(value):
    first = value.astype(jnp.bfloat16).astype(jnp.float32)
    rest = value - first
    second = rest.astype(jnp.bfloat16).astype(jnp.float32)
    return first, second, rest - second


def offsets():
    return [(a, b, c) for a in (-1, 0, 1) for b in (-1, 0, 1) for c in (-1, 0, 1)]


def kind_at(offset, count):
    if count >= 3:
        return offset + 1
    return abs(offset) if count == 2 else 0


def place_at(offset, sizes):
    i, j, k = (kind_at(o, n) for o, n in zip(offset, sizes))
    return (i * kinds(sizes[1]) + j) * kinds(sizes[2]) + k


def role_places(role, sizes):
    places = [place_at(o, sizes) for o in offsets() if (o[0] != 0, o[1] != 0) == (role >= 2, role % 2 == 1)]
    return sorted(set(places))


def role_slots(role):
    return [n for n, o in enumerate(offsets()) if (o[0] != 0, o[1] != 0) == (role >= 2, role % 2 == 1)]


def gas_features(gas, feat, slot, offset):
    tiles = gas[3].shape[0]
    px, py, pz = (gas[k] + (offset[k] - 0.5) for k in range(3))
    root = lax.rsqrt(gas[3])
    square = (px * px + py * py + pz * pz) * root
    base = [n for role in range(4) for n in role_slots(role)].index(slot) * tiles
    for comp, value in enumerate((px * root, py * root, pz * root, square, root)):
        for part, piece in enumerate(split3(value)):
            at = (part * 5 + comp) * 128
            feat[base : base + tiles, at : at + 128] = piece.astype(jnp.bfloat16)


def source_features(pos, radius, rows, left):
    blocks = pos.shape[1]
    r = radius[...]
    inv = 1.0 / (r * r)
    sx, sy, sz = (pos[k] - 0.5 for k in range(3))
    comps = [-2.0 * inv * sx, -2.0 * inv * sy, -2.0 * inv * sz, inv, 1.0 + inv * (sx * sx + sy * sy + sz * sz)]
    parts = [split3(v) for v in comps]
    zero = jnp.zeros_like(r)
    for group in range(3):
        for part in range(3):
            for comp in range(5):
                value = parts[comp][group] if part + group < 3 else zero
                rows[pl.ds(group * PARTS + part * 5 + comp, blocks, stride=3 * PARTS), :] = value
        rows[pl.ds(group * PARTS + 15, blocks, stride=3 * PARTS), :] = zero
    for b in range(blocks):
        left[b] = rows[b * 3 * PARTS : (b + 1) * 3 * PARTS, :].T.astype(jnp.bfloat16)


def over_blocks(blocks, unroll, body):
    def step(i, carry):
        for k in range(unroll):
            body(i * unroll + k)
        return carry

    lax.fori_loop(0, blocks // unroll, step, 0)


def gather(role, tiles, feat, hot_in, picked):
    slots = [n for r in range(4) for n in role_slots(r)]
    first = slots.index(role_slots(role)[0]) * tiles
    depth = len(role_slots(role)) * tiles
    pairs = hot_in.shape[1]
    got = jnp.dot(hot_in[role, :, 0:depth], feat[first : first + depth, :], preferred_element_type=jnp.float32)
    for row in range(PARTS - 1):
        picked[role % 2, pl.ds(row, pairs, stride=PARTS), :] = got[:, row * 128 : row * 128 + 128]


def weigh(role, picked, left, weights, sums, norms, unroll):
    blocks = left.shape[0]

    def body(b):
        near = []
        for z in range(2):
            at = pl.multiple_of((z * blocks + b) * PARTS, PARTS)
            near.append(picked[role % 2, pl.ds(at, PARTS), :].astype(jnp.bfloat16))
        rhs = jnp.concatenate([jnp.concatenate(near, axis=1)] * 3, axis=0)
        u = jnp.dot(left[b], rhs, preferred_element_type=jnp.float32)
        w = 1.0 / (u * u)
        part = w[:, :128] + w[:, 128:]
        if role:
            part = sums[b] + part
        if role < 3:
            sums[b] = part
        else:
            norms[pl.ds(b, 1), :] = jnp.sum(part.T, axis=0, keepdims=True)
        w1 = w.astype(jnp.bfloat16)
        weights[role, b, 0:128] = w1
        weights[role, b, 128:256] = (w - w1.astype(jnp.float32)).astype(jnp.bfloat16)

    over_blocks(blocks, unroll, body)


def normalise(count, norms, yields, momentum, loads):
    blocks = norms.shape[0]
    lane = lax.broadcasted_iota(jnp.int32, (blocks, 128), 1)
    index = lax.broadcasted_iota(jnp.int32, (blocks, 128), 0) * 128 + lane
    scale = jnp.where(index < count[0, 0], 1.0, 0.0) / norms[...]
    zero = jnp.zeros_like(scale)
    for q, value in enumerate([yields[0], momentum[0], momentum[1], momentum[2], yields[1], zero, zero, zero]):
        coef = value * scale
        high = coef.astype(jnp.bfloat16).astype(jnp.float32)
        loads[pl.ds(q, blocks, stride=16), :] = high
        loads[pl.ds(q + 8, blocks, stride=16), :] = coef - high


def deposit(role, loads, weights, moved, unroll):
    blocks = weights.shape[1]

    def body(b):
        half = loads[pl.ds(pl.multiple_of(b * 16, 16), 16), :].astype(jnp.bfloat16)
        got = jnp.dot(jnp.concatenate([half, half], axis=1), weights[role, b], preferred_element_type=jnp.float32)
        both = got[0:8] + got[8:16]
        for z in range(2):
            start = pl.multiple_of((z * blocks + b) * 8, 8)
            moved[role, pl.ds(start, 8), :] = both[:, z * 128 : z * 128 + 128]

    over_blocks(blocks, unroll, body)


def one_hots(sizes, tiles, table_rows, hot_in, hot_out):
    nx, ny, nz = sizes
    ids = table_rows[...]
    slot, tile = ids // tiles, ids % tiles
    at = kind_of(slot // 9 - 1, nx) * kinds(ny) + kind_of(slot // 3 % 3 - 1, ny)
    at = (at * kinds(nz) + kind_of(slot % 3 - 1, nz)) * tiles + tile
    flip_a = slot[0:1] // 9 == 0
    flip_b = slot[0:1] // 3 % 3 == 0

    def pick(values, role):
        row = []
        for z in range(2):
            low, high = (
                jnp.where(flip_b, values[4 * a + z + 2 : 4 * a + z + 3], values[4 * a + z : 4 * a + z + 1])
                if role % 2 == 0
                else jnp.where(flip_b, values[4 * a + z : 4 * a + z + 1], values[4 * a + z + 2 : 4 * a + z + 3])
                for a in range(2)
            )
            row.append(jnp.where(flip_a, high, low) if role < 2 else jnp.where(flip_a, low, high))
        return jnp.concatenate(row, axis=1)

    for role in range(4):
        source, target = pick(ids, role), pick(at, role)
        pairs = source.shape[1]
        index = lax.broadcasted_iota(jnp.int32, (tiles, pairs), 0)
        hot = [(index + n * tiles == source).astype(jnp.float32) for n in role_slots(role)]
        depth = len(hot) * tiles
        hot_in[role, :, 0:depth] = jnp.concatenate(hot, axis=0).T.astype(jnp.bfloat16)
        hot = [(index + n * tiles == target).astype(jnp.float32) for n in role_places(role, sizes)]
        hot = jnp.concatenate(hot, axis=0).astype(jnp.bfloat16)
        hot_out[role, 0 : hot.shape[0], :] = jnp.concatenate([hot, hot], axis=1)


def scatter(role, sizes, hot_out, moved, out, done):
    tiles = out.shape[2]
    places = role_places(role, sizes)
    pairs = hot_out.shape[2] // 2
    values = jnp.concatenate([moved[role, pl.ds(q, pairs, stride=8), :] for q in range(5)], axis=1)
    m1 = values.astype(jnp.bfloat16)
    m2 = (values - m1.astype(jnp.float32)).astype(jnp.bfloat16)
    hot = hot_out[role, 0 : len(places) * tiles, :]
    got = jnp.dot(hot, jnp.concatenate([m1, m2], axis=0), preferred_element_type=jnp.float32)
    for n, place in enumerate(places):
        for q in range(5):
            value = got[n * tiles : (n + 1) * tiles, q * 128 : (q + 1) * 128]
            out[place, q] = out[place, q] + value if place in done else value
        done.add(place)


def core_scratch(blocks, tiles):
    return [
        pltpu.VMEM((27 * tiles, (PARTS - 1) * 128), jnp.bfloat16),
        pltpu.VMEM((blocks * 3 * PARTS, 128), jnp.float32),
        pltpu.VMEM((blocks, 128, 3 * PARTS), jnp.bfloat16),
        pltpu.VMEM((4, blocks, 256, 256), jnp.bfloat16),
        pltpu.VMEM((blocks, 128, 128), jnp.float32),
        pltpu.VMEM((blocks, 128), jnp.float32),
        pltpu.VMEM((blocks * 16, 128), jnp.float32),
        pltpu.VMEM((4, blocks * 16, 128), jnp.float32),
        pltpu.VMEM((4, 2 * blocks, 12 * tiles), jnp.bfloat16),
        pltpu.VMEM((4, 12 * tiles, 4 * blocks), jnp.bfloat16),
        pltpu.VMEM((2, 2 * blocks * PARTS, 128), jnp.float32),
    ]


def fused_kernel(sizes, pos, mass, table, count, spos, sradius, syield, smomentum, out, *scratch):
    (near, count_s, table_v, pos_v, radius_v, yield_v, momentum_v, deposits, part, got_z, got) = scratch[:11]
    (feat, rows, left, weights, sums, norms, loads, moved, hot_in, hot_out, picked) = scratch[11:22]
    local_sem, send_sem, recv_sem, gsend_z, grecv_z, gsend, grecv = scratch[22:]
    nx, ny, nz = sizes
    own = tuple(own_kind(n) for n in sizes)
    tiles = near.shape[2]
    blocks = pos_v.shape[1]
    unroll = math.gcd(blocks, 16)

    def place(i, j, k):
        return (i * kinds(ny) + j) * kinds(nz) + k

    home = place(*own)
    gas_in = [
        pltpu.make_async_copy(pos, near.at[home, pl.ds(0, 3)], local_sem.at[0]),
        pltpu.make_async_copy(mass, near.at[home, pl.ds(3, 1)], local_sem.at[1]),
    ]
    pairs = [(spos, pos_v), (sradius, radius_v), (syield, yield_v), (smomentum, momentum_v)]
    pairs += [(count, count_s), (table, table_v)]
    rest_in = [pltpu.make_async_copy(src, dst, local_sem.at[2 + n]) for n, (src, dst) in enumerate(pairs)]
    for copy in gas_in + rest_in:
        copy.start()

    def features(i, j, k):
        for slot, offset in enumerate(offsets()):
            if place_at(offset, sizes) == place(i, j, k):
                gas_features([near[place(i, j, k), c] for c in range(4)], feat, slot, offset)

    def meanwhile():
        for copy in gas_in + rest_in:
            copy.wait()
        source_features(pos_v, radius_v, rows, left)
        one_hots(sizes, tiles, table_v, hot_in, hot_out)
        spare = jnp.zeros((2 * blocks, 128), jnp.float32)
        for side in range(2):
            picked[side, pl.ds(PARTS - 1, 2 * blocks, stride=PARTS), :] = spare
        features(*own)

    greet(sizes, meanwhile)
    finished = []

    def gas_copy(source, target, device):
        return pltpu.make_async_remote_copy(
            src_ref=near.at[source],
            dst_ref=near.at[target],
            send_sem=send_sem.at[target],
            recv_sem=recv_sem.at[target],
            device_id=device,
            device_id_type=MESH,
        )

    def send(source, target, device):
        copy = gas_copy(source, target, device)
        copy.start()
        finished.append(copy)

    def arrived(i, j, k):
        target = place(i, j, k)
        gas_copy(target, target, next(iter(cores_of(sizes) + columns_of(sizes)))[1]).wait_recv()

    def to_cores(i, j):
        for k, device in cores_of(sizes):
            send(place(i, j, own[2]), place(i, j, facing(k, nz)), device)

    columns = columns_of(sizes)
    far = far_first(sizes)
    for (i, j), device in far:
        send(home, place(facing_at(i, nx), facing_at(j, ny), own[2]), device)
    to_cores(own[0], own[1])
    def weigh_role(role):
        gather(role, tiles, feat, hot_in, picked)
        weigh(role, picked, left, weights, sums, norms, unroll)

    for k, _ in steps_of(nz):
        arrived(own[0], own[1], k)
        features(own[0], own[1], k)
    weigh_role(0)
    def sides(role):
        return [at for at, _ in columns if 2 * (at[0] != own[0]) + (at[1] != own[1]) == role]

    def take(role):
        for at in sides(role):
            arrived(at[0], at[1], own[2])
            to_cores(*at)
            pass

    def early(role):
        for at in sides(role):
            features(at[0], at[1], own[2])

    def finish(role):
        for i, j in sides(role):
            for k, _ in steps_of(nz):
                arrived(i, j, k)
                features(i, j, k)
        weigh_role(role)

    take(1)
    take(2)
    take(3)
    early(1)
    early(2)
    early(3)
    finish(1)
    finish(2)
    finish(3)
    normalise(count_s, norms, yield_v, momentum_v, loads)
    done = set()

    def gain_copy(src, dst, send_at, recv_at, device):
        return pltpu.make_async_remote_copy(
            src_ref=src, dst_ref=dst, send_sem=send_at, recv_sem=recv_at, device_id=device, device_id_type=MESH
        )

    def z_copy(i, j, k, device):
        at = place(i, j, k)
        return gain_copy(deposits.at[at], got_z.at[at], gsend_z.at[at], grecv_z.at[at], device)

    def side_copy(i, j, device):
        at = i * kinds(ny) + j
        return gain_copy(part.at[at], got.at[at], gsend.at[at], grecv.at[at], device)

    def start(copy):
        copy.start()
        finished.append(copy)

    def column_total(i, j):
        total = deposits[place(i, j, own[2])]
        for k, device in cores_of(sizes):
            z_copy(i, j, k, device).wait_recv()
            total = total + got_z[place(i, j, k)]
        return total

    def role_columns(role):
        return [c for c, r in zip(far, far_roles(sizes)) if r == role]

    waiting = []

    def flush():
        while waiting:
            start(waiting.pop(0))

    def totals(role):
        for (i, j), device in role_columns(role):
            part[i * kinds(ny) + j] = column_total(i, j)
            flush()
            waiting.append(side_copy(i, j, device))

    for role in (3, 2, 1, 0):
        deposit(role, loads, weights, moved, unroll)
        flush()
        scatter(role, sizes, hot_out, moved, deposits, done)
        for (i, j), _ in role_columns(role) if role else [(own[:2], None)]:
            for k, device in cores_of(sizes):
                start(z_copy(i, j, k, device))
        if role < 3:
            totals(role + 1)
    flush()
    total = column_total(*own[:2])
    for (i, j), device in columns:
        side_copy(i, j, device).wait_recv()
        total = total + got[i * kinds(ny) + j]
    out[...] = total / near[home, 3]
    for copy in finished:
        copy.wait_send()


def local(sizes, gas_pos, gas_mass, source_pos, source_radius, source_yield, source_momentum, source_tiles, source_count):
    gas_size = gas_pos.shape[-1]
    tiles = gas_size // 128
    blocks = source_pos.shape[-1] // 128
    listed = source_tiles.shape[-1]
    slots = kinds(sizes[0]) * kinds(sizes[1]) * kinds(sizes[2])
    sides = kinds(sizes[0]) * kinds(sizes[1])
    piece = (5, tiles, 128)
    given = pl.BlockSpec(memory_space=pltpu.HBM)
    dma = pltpu.SemaphoreType.DMA
    gain = pl.pallas_call(
        functools.partial(fused_kernel, sizes),
        out_shape=pltpu.VMEM(piece, jnp.float32),
        in_specs=[given] * 8,
        out_specs=pl.BlockSpec(memory_space=pltpu.VMEM),
        scratch_shapes=[
            pltpu.VMEM((slots, 4, tiles, 128), jnp.float32),
            pltpu.SMEM((1, 1), jnp.int32),
            pltpu.VMEM((listed, blocks), jnp.int32),
            pltpu.VMEM((3, blocks, 128), jnp.float32),
            pltpu.VMEM((blocks, 128), jnp.float32),
            pltpu.VMEM((2, blocks, 128), jnp.float32),
            pltpu.VMEM((3, blocks, 128), jnp.float32),
            pltpu.VMEM((slots, *piece), jnp.float32),
            pltpu.VMEM((sides, *piece), jnp.float32),
            pltpu.VMEM((slots, *piece), jnp.float32),
            pltpu.VMEM((sides, *piece), jnp.float32),
            *core_scratch(blocks, tiles),
            dma((8,)),
            dma((slots,)),
            dma((slots,)),
            dma((slots,)),
            dma((slots,)),
            dma((sides,)),
            dma((sides,)),
        ],
        compiler_params=pltpu.CompilerParams(collective_id=0, has_side_effects=True, vmem_limit_bytes=LIMIT),
    )(
        gas_pos.reshape(3, tiles, 128),
        gas_mass.reshape(1, tiles, 128),
        source_tiles.reshape(blocks, listed).T,
        source_count.reshape(1, 1),
        source_pos.reshape(3, blocks, 128),
        source_radius.reshape(blocks, 128),
        source_yield.reshape(2, blocks, 128),
        source_momentum.reshape(3, blocks, 128),
    )
    return gain.reshape(5, 1, 1, 1, gas_size)


def solution(mesh):
    sizes = (mesh.shape["gx"], mesh.shape["gy"], mesh.shape["gz"])
    in_specs = (
        P(None, "gx", "gy", "gz", None),
        P("gx", "gy", "gz", None),
        P(None, "gx", "gy", "gz", None),
        P("gx", "gy", "gz", None),
        P(None, "gx", "gy", "gz", None),
        P(None, "gx", "gy", "gz", None),
        P("gx", "gy", "gz", None, None),
        P("gx", "gy", "gz"),
    )
    out_specs = P(None, "gx", "gy", "gz", None)
    return jax.shard_map(
        functools.partial(local, sizes), mesh=mesh, in_specs=in_specs, out_specs=out_specs, check_vma=False
    )
```

```python
import functools
import math

import jax
import jax.numpy as jnp
from jax import lax
from jax.experimental import pallas as pl
from jax.experimental.pallas import tpu as pltpu
from jax.sharding import PartitionSpec as P


def kinds(count):
    return min(count, 3)


def kind_of(offset, count):
    if count >= 3:
        return offset + 1
    if count == 2:
        return jnp.abs(offset)
    return offset * 0


def own_kind(count):
    return 1 if count >= 3 else 0


def steps_of(count):
    if count >= 3:
        return ((0, -1), (2, 1))
    return ((1, 1),) if count == 2 else ()


MESH = pl.DeviceIdType.MESH
LIMIT = 67_043_328 - 64 * 1024


def shifted(axis, count, step):
    return lax.rem(lax.axis_index(axis) + step + count, count)


def columns_of(sizes):
    nx, ny, _ = sizes
    choices_x = steps_of(nx) + ((own_kind(nx), 0),)
    choices_y = ((own_kind(ny), 0),) + steps_of(ny)
    return [
        ((i, j), {"gx": shifted("gx", nx, dx), "gy": shifted("gy", ny, dy)})
        for i, dx in choices_x
        for j, dy in choices_y
        if dx or dy
    ]


def far_first(sizes):
    nx, ny, _ = sizes
    turn_x = 2 * lax.rem(lax.axis_index("gx"), 2) - 1
    turn_y = jnp.where(lax.axis_index("gy") == 0, -1, 1)
    choices_x = [(1 + turn_x, turn_x), (1 - turn_x, -turn_x)] if nx >= 3 else list(steps_of(nx))
    choices_y = [(1 + turn_y, turn_y), (1 - turn_y, -turn_y)] if ny >= 3 else list(steps_of(ny))
    own_x, own_y = (own_kind(nx), 0), (own_kind(ny), 0)
    order = [(x, y) for y in choices_y for x in choices_x + [own_x]] + [(x, own_y) for x in choices_x]
    return [((i, j), {"gx": shifted("gx", nx, dx), "gy": shifted("gy", ny, dy)}) for (i, dx), (j, dy) in order]


def far_roles(sizes):
    steps_x, steps_y = len(steps_of(sizes[0])), len(steps_of(sizes[1]))
    return ([3] * steps_x + [1]) * steps_y + [2] * steps_x


def facing_at(kind, count):
    return 2 - kind if count >= 3 else kind


def cores_of(sizes):
    return [(k, {"gz": shifted("gz", sizes[2], dz)}) for k, dz in steps_of(sizes[2])]


def greet(sizes, meanwhile):
    barrier = pltpu.get_barrier_semaphore()
    own = (own_kind(sizes[0]), own_kind(sizes[1]))
    peers = [c for c in columns_of(sizes) if c[0][0] == own[0] or c[0][1] == own[1]] + cores_of(sizes)
    for _, device in peers:
        pl.semaphore_signal(barrier, inc=1, device_id=device, device_id_type=MESH)
    meanwhile()
    if peers:
        pl.semaphore_wait(barrier, len(peers))


def facing(kind, count):
    return 2 - kind if count >= 3 else kind


PARTS = 16


def split3(value):
    first = value.astype(jnp.bfloat16).astype(jnp.float32)
    rest = value - first
    second = rest.astype(jnp.bfloat16).astype(jnp.float32)
    return first, second, rest - second


def offsets():
    return [(a, b, c) for a in (-1, 0, 1) for b in (-1, 0, 1) for c in (-1, 0, 1)]


def kind_at(offset, count):
    if count >= 3:
        return offset + 1
    return abs(offset) if count == 2 else 0


def place_at(offset, sizes):
    i, j, k = (kind_at(o, n) for o, n in zip(offset, sizes))
    return (i * kinds(sizes[1]) + j) * kinds(sizes[2]) + k


def role_places(role, sizes):
    places = [place_at(o, sizes) for o in offsets() if (o[0] != 0, o[1] != 0) == (role >= 2, role % 2 == 1)]
    return sorted(set(places))


def role_slots(role):
    return [n for n, o in enumerate(offsets()) if (o[0] != 0, o[1] != 0) == (role >= 2, role % 2 == 1)]


def gas_features(gas, feat, slot, offset):
    tiles = gas[3].shape[0]
    px, py, pz = (gas[k] + (offset[k] - 0.5) for k in range(3))
    root = lax.rsqrt(gas[3])
    square = (px * px + py * py + pz * pz) * root
    base = [n for role in range(4) for n in role_slots(role)].index(slot) * tiles
    for comp, value in enumerate((px * root, py * root, pz * root, square, root)):
        for part, piece in enumerate(split3(value)):
            at = (part * 5 + comp) * 128
            feat[base : base + tiles, at : at + 128] = piece.astype(jnp.bfloat16)


def source_features(pos, radius, rows, left):
    blocks = pos.shape[1]
    r = radius[...]
    inv = 1.0 / (r * r)
    sx, sy, sz = (pos[k] - 0.5 for k in range(3))
    comps = [-2.0 * inv * sx, -2.0 * inv * sy, -2.0 * inv * sz, inv, 1.0 + inv * (sx * sx + sy * sy + sz * sz)]
    parts = [split3(v) for v in comps]
    zero = jnp.zeros_like(r)
    for group in range(3):
        for part in range(3):
            for comp in range(5):
                value = parts[comp][group] if part + group < 3 else zero
                rows[pl.ds(group * PARTS + part * 5 + comp, blocks, stride=3 * PARTS), :] = value
        rows[pl.ds(group * PARTS + 15, blocks, stride=3 * PARTS), :] = zero
    for b in range(blocks):
        left[b] = rows[b * 3 * PARTS : (b + 1) * 3 * PARTS, :].T.astype(jnp.bfloat16)


def over_blocks(blocks, unroll, body):
    def step(i, carry):
        for k in range(unroll):
            body(i * unroll + k)
        return carry

    lax.fori_loop(0, blocks // unroll, step, 0)


def gather(role, tiles, feat, hot_in, picked):
    slots = [n for r in range(4) for n in role_slots(r)]
    first = slots.index(role_slots(role)[0]) * tiles
    depth = len(role_slots(role)) * tiles
    pairs = hot_in.shape[1]
    got = jnp.dot(hot_in[role, :, 0:depth], feat[first : first + depth, :], preferred_element_type=jnp.float32)
    for row in range(PARTS - 1):
        picked[role, pl.ds(row, pairs, stride=PARTS), :] = got[:, row * 128 : row * 128 + 128]


def weigh(role, picked, left, weights, sums, norms, unroll):
    blocks = left.shape[0]

    def body(b):
        near = []
        for z in range(2):
            at = pl.multiple_of((z * blocks + b) * PARTS, PARTS)
            near.append(picked[role, pl.ds(at, PARTS), :].astype(jnp.bfloat16))
        rhs = jnp.concatenate([jnp.concatenate(near, axis=1)] * 3, axis=0)
        u = jnp.dot(left[b], rhs, preferred_element_type=jnp.float32)
        w = 1.0 / (u * u)
        part = w[:, :128] + w[:, 128:]
        if role:
            part = sums[b] + part
        if role < 3:
            sums[b] = part
        else:
            norms[pl.ds(b, 1), :] = jnp.sum(part.T, axis=0, keepdims=True)
        w1 = w.astype(jnp.bfloat16)
        weights[role, b, 0:128] = w1
        weights[role, b, 128:256] = (w - w1.astype(jnp.float32)).astype(jnp.bfloat16)

    over_blocks(blocks, unroll, body)


def normalise(count, norms, yields, momentum, loads):
    blocks = norms.shape[0]
    lane = lax.broadcasted_iota(jnp.int32, (blocks, 128), 1)
    index = lax.broadcasted_iota(jnp.int32, (blocks, 128), 0) * 128 + lane
    scale = jnp.where(index < count[0, 0], 1.0, 0.0) / norms[...]
    zero = jnp.zeros_like(scale)
    for q, value in enumerate([yields[0], momentum[0], momentum[1], momentum[2], yields[1], zero, zero, zero]):
        coef = value * scale
        high = coef.astype(jnp.bfloat16).astype(jnp.float32)
        loads[pl.ds(q, blocks, stride=16), :] = high
        loads[pl.ds(q + 8, blocks, stride=16), :] = coef - high


def deposit(role, loads, weights, moved, unroll):
    blocks = weights.shape[1]

    def body(b):
        half = loads[pl.ds(pl.multiple_of(b * 16, 16), 16), :].astype(jnp.bfloat16)
        got = jnp.dot(jnp.concatenate([half, half], axis=1), weights[role, b], preferred_element_type=jnp.float32)
        both = got[0:8] + got[8:16]
        for z in range(2):
            start = pl.multiple_of((z * blocks + b) * 8, 8)
            moved[role, pl.ds(start, 8), :] = both[:, z * 128 : z * 128 + 128]

    over_blocks(blocks, unroll, body)


def one_hots(sizes, tiles, table_rows, hot_in, hot_out):
    nx, ny, nz = sizes
    ids = table_rows[...]
    slot, tile = ids // tiles, ids % tiles
    at = kind_of(slot // 9 - 1, nx) * kinds(ny) + kind_of(slot // 3 % 3 - 1, ny)
    at = (at * kinds(nz) + kind_of(slot % 3 - 1, nz)) * tiles + tile
    flip_a = slot[0:1] // 9 == 0
    flip_b = slot[0:1] // 3 % 3 == 0

    def pick(values, role):
        row = []
        for z in range(2):
            low, high = (
                jnp.where(flip_b, values[4 * a + z + 2 : 4 * a + z + 3], values[4 * a + z : 4 * a + z + 1])
                if role % 2 == 0
                else jnp.where(flip_b, values[4 * a + z : 4 * a + z + 1], values[4 * a + z + 2 : 4 * a + z + 3])
                for a in range(2)
            )
            row.append(jnp.where(flip_a, high, low) if role < 2 else jnp.where(flip_a, low, high))
        return jnp.concatenate(row, axis=1)

    for role in range(4):
        source, target = pick(ids, role), pick(at, role)
        pairs = source.shape[1]
        index = lax.broadcasted_iota(jnp.int32, (tiles, pairs), 0)
        hot = [(index + n * tiles == source).astype(jnp.float32) for n in role_slots(role)]
        depth = len(hot) * tiles
        hot_in[role, :, 0:depth] = jnp.concatenate(hot, axis=0).T.astype(jnp.bfloat16)
        hot = [(index + n * tiles == target).astype(jnp.float32) for n in role_places(role, sizes)]
        hot = jnp.concatenate(hot, axis=0).astype(jnp.bfloat16)
        hot_out[role, 0 : hot.shape[0], :] = jnp.concatenate([hot, hot], axis=1)


def scatter(role, sizes, hot_out, moved, out, done):
    tiles = out.shape[2]
    places = role_places(role, sizes)
    pairs = hot_out.shape[2] // 2
    values = jnp.concatenate([moved[role, pl.ds(q, pairs, stride=8), :] for q in range(5)], axis=1)
    m1 = values.astype(jnp.bfloat16)
    m2 = (values - m1.astype(jnp.float32)).astype(jnp.bfloat16)
    hot = hot_out[role, 0 : len(places) * tiles, :]
    got = jnp.dot(hot, jnp.concatenate([m1, m2], axis=0), preferred_element_type=jnp.float32)
    for n, place in enumerate(places):
        for q in range(5):
            value = got[n * tiles : (n + 1) * tiles, q * 128 : (q + 1) * 128]
            out[place, q] = out[place, q] + value if place in done else value
        done.add(place)


def core_scratch(blocks, tiles):
    return [
        pltpu.VMEM((27 * tiles, (PARTS - 1) * 128), jnp.bfloat16),
        pltpu.VMEM((blocks * 3 * PARTS, 128), jnp.float32),
        pltpu.VMEM((blocks, 128, 3 * PARTS), jnp.bfloat16),
        pltpu.VMEM((4, blocks, 256, 256), jnp.bfloat16),
        pltpu.VMEM((blocks, 128, 128), jnp.float32),
        pltpu.VMEM((blocks, 128), jnp.float32),
        pltpu.VMEM((blocks * 16, 128), jnp.float32),
        pltpu.VMEM((4, blocks * 16, 128), jnp.float32),
        pltpu.VMEM((4, 2 * blocks, 12 * tiles), jnp.bfloat16),
        pltpu.VMEM((4, 12 * tiles, 4 * blocks), jnp.bfloat16),
        pltpu.VMEM((4, 2 * blocks * PARTS, 128), jnp.float32),
    ]


def fused_kernel(sizes, pos, mass, table, count, spos, sradius, syield, smomentum, out, *scratch):
    (near, count_s, table_v, pos_v, radius_v, yield_v, momentum_v, deposits, part, got_z, got) = scratch[:11]
    (feat, rows, left, weights, sums, norms, loads, moved, hot_in, hot_out, picked) = scratch[11:22]
    local_sem, send_sem, recv_sem, gsend_z, grecv_z, gsend, grecv, ready_sem = scratch[22:]
    nx, ny, nz = sizes
    own = tuple(own_kind(n) for n in sizes)
    tiles = near.shape[2]
    blocks = pos_v.shape[1]
    unroll = math.gcd(blocks, 16)

    def place(i, j, k):
        return (i * kinds(ny) + j) * kinds(nz) + k

    home = place(*own)
    gas_in = [
        pltpu.make_async_copy(pos, near.at[home, pl.ds(0, 3)], local_sem.at[0]),
        pltpu.make_async_copy(mass, near.at[home, pl.ds(3, 1)], local_sem.at[1]),
    ]
    pairs = [(spos, pos_v), (sradius, radius_v), (syield, yield_v), (smomentum, momentum_v)]
    pairs += [(count, count_s), (table, table_v)]
    rest_in = [pltpu.make_async_copy(src, dst, local_sem.at[2 + n]) for n, (src, dst) in enumerate(pairs)]
    for copy in gas_in + rest_in:
        copy.start()

    def features(i, j, k):
        for slot, offset in enumerate(offsets()):
            if place_at(offset, sizes) == place(i, j, k):
                gas_features([near[place(i, j, k), c] for c in range(4)], feat, slot, offset)

    def meanwhile():
        for copy in gas_in + rest_in:
            copy.wait()
        source_features(pos_v, radius_v, rows, left)
        one_hots(sizes, tiles, table_v, hot_in, hot_out)
        spare = jnp.zeros((2 * blocks, 128), jnp.float32)
        for side in range(4):
            picked[side, pl.ds(PARTS - 1, 2 * blocks, stride=PARTS), :] = spare
        features(*own)

    greet(sizes, meanwhile)
    finished = []

    def gas_copy(source, target, device):
        return pltpu.make_async_remote_copy(
            src_ref=near.at[source],
            dst_ref=near.at[target],
            send_sem=send_sem.at[target],
            recv_sem=recv_sem.at[target],
            device_id=device,
            device_id_type=MESH,
        )

    def send(source, target, device):
        copy = gas_copy(source, target, device)
        copy.start()
        finished.append(copy)

    def arrived(i, j, k):
        target = place(i, j, k)
        gas_copy(target, target, next(iter(cores_of(sizes) + columns_of(sizes)))[1]).wait_recv()

    def to_cores(i, j):
        for k, device in cores_of(sizes):
            send(place(i, j, own[2]), place(i, j, facing(k, nz)), device)

    columns = columns_of(sizes)
    far = list(zip(far_first(sizes), far_roles(sizes)))
    others = [device for at, device in columns if at[0] != own[0] and at[1] == own[1]]
    corners = [device for at, device in columns if at[0] != own[0] and at[1] != own[1]]
    if corners:
        for device in others:
            pl.semaphore_signal(ready_sem, inc=1, device_id=device, device_id_type=MESH)

    def send_home(roles):
        for ((i, j), device), role in far:
            if role in roles:
                send(home, place(facing_at(i, nx), facing_at(j, ny), own[2]), device)

    def ready():
        if corners:
            pl.semaphore_wait(ready_sem, len(others))
        send_home((3,))

    send_home((1, 2))
    to_cores(own[0], own[1])

    def weigh_role(role):
        gather(role, tiles, feat, hot_in, picked)
        weigh(role, picked, left, weights, sums, norms, unroll)

    def sides(role):
        return [at for at, _ in columns if 2 * (at[0] != own[0]) + (at[1] != own[1]) == role]

    def take(role):
        for at in sides(role):
            arrived(at[0], at[1], own[2])
            to_cores(*at)
            pass

    def early(role):
        for at in sides(role):
            features(at[0], at[1], own[2])

    def finish(role):
        for i, j in sides(role):
            for k, _ in steps_of(nz):
                arrived(i, j, k)
                features(i, j, k)
        weigh_role(role)

    def received(role):
        for i, j in sides(role):
            for k, _ in steps_of(nz):
                arrived(i, j, k)
                features(i, j, k)

    def pick(role):
        gather(role, tiles, feat, hot_in, picked)

    def weight(role):
        weigh(role, picked, left, weights, sums, norms, unroll)

    ready()
    for k, _ in steps_of(nz):
        arrived(own[0], own[1], k)
        features(own[0], own[1], k)
    pick(0)
    weight(0)
    take(1)
    take(2)
    early(1)
    early(2)
    received(1)
    pick(1)
    received(2)
    pick(2)
    weight(1)
    weight(2)
    take(3)
    early(3)
    received(3)
    pick(3)
    weight(3)
    normalise(count_s, norms, yield_v, momentum_v, loads)
    done = set()

    def gain_copy(src, dst, send_at, recv_at, device):
        return pltpu.make_async_remote_copy(
            src_ref=src, dst_ref=dst, send_sem=send_at, recv_sem=recv_at, device_id=device, device_id_type=MESH
        )

    def z_copy(i, j, k, device):
        at = place(i, j, k)
        return gain_copy(deposits.at[at], got_z.at[at], gsend_z.at[at], grecv_z.at[at], device)

    def side_copy(i, j, device):
        at = i * kinds(ny) + j
        return gain_copy(part.at[at], got.at[at], gsend.at[at], grecv.at[at], device)

    def start(copy):
        copy.start()
        finished.append(copy)

    def column_total(i, j):
        total = deposits[place(i, j, own[2])]
        for k, device in cores_of(sizes):
            z_copy(i, j, k, device).wait_recv()
            total = total + got_z[place(i, j, k)]
        return total

    def role_columns(role):
        return [c for c, r in far if r == role]

    waiting = []

    def flush():
        while waiting:
            start(waiting.pop(0))

    def totals(role):
        for (i, j), device in role_columns(role):
            part[i * kinds(ny) + j] = column_total(i, j)
            flush()
            waiting.append(side_copy(i, j, device))

    for role in (3, 2, 1, 0):
        deposit(role, loads, weights, moved, unroll)
        flush()
        scatter(role, sizes, hot_out, moved, deposits, done)
        for (i, j), _ in role_columns(role) if role else [(own[:2], None)]:
            for k, device in cores_of(sizes):
                start(z_copy(i, j, k, device))
        if role < 3:
            totals(role + 1)
    flush()
    total = column_total(*own[:2])
    for (i, j), device in columns:
        side_copy(i, j, device).wait_recv()
        total = total + got[i * kinds(ny) + j]
    out[...] = total / near[home, 3]
    for copy in finished:
        copy.wait_send()


def local(sizes, gas_pos, gas_mass, source_pos, source_radius, source_yield, source_momentum, source_tiles, source_count):
    gas_size = gas_pos.shape[-1]
    tiles = gas_size // 128
    blocks = source_pos.shape[-1] // 128
    listed = source_tiles.shape[-1]
    slots = kinds(sizes[0]) * kinds(sizes[1]) * kinds(sizes[2])
    sides = kinds(sizes[0]) * kinds(sizes[1])
    piece = (5, tiles, 128)
    given = pl.BlockSpec(memory_space=pltpu.HBM)
    dma = pltpu.SemaphoreType.DMA
    gain = pl.pallas_call(
        functools.partial(fused_kernel, sizes),
        out_shape=pltpu.VMEM(piece, jnp.float32),
        in_specs=[given] * 8,
        out_specs=pl.BlockSpec(memory_space=pltpu.VMEM),
        scratch_shapes=[
            pltpu.VMEM((slots, 4, tiles, 128), jnp.float32),
            pltpu.SMEM((1, 1), jnp.int32),
            pltpu.VMEM((listed, blocks), jnp.int32),
            pltpu.VMEM((3, blocks, 128), jnp.float32),
            pltpu.VMEM((blocks, 128), jnp.float32),
            pltpu.VMEM((2, blocks, 128), jnp.float32),
            pltpu.VMEM((3, blocks, 128), jnp.float32),
            pltpu.VMEM((slots, *piece), jnp.float32),
            pltpu.VMEM((sides, *piece), jnp.float32),
            pltpu.VMEM((slots, *piece), jnp.float32),
            pltpu.VMEM((sides, *piece), jnp.float32),
            *core_scratch(blocks, tiles),
            dma((8,)),
            dma((slots,)),
            dma((slots,)),
            dma((slots,)),
            dma((slots,)),
            dma((sides,)),
            dma((sides,)),
            pltpu.SemaphoreType.REGULAR,
        ],
        compiler_params=pltpu.CompilerParams(collective_id=0, has_side_effects=True, vmem_limit_bytes=LIMIT),
    )(
        gas_pos.reshape(3, tiles, 128),
        gas_mass.reshape(1, tiles, 128),
        source_tiles.reshape(blocks, listed).T,
        source_count.reshape(1, 1),
        source_pos.reshape(3, blocks, 128),
        source_radius.reshape(blocks, 128),
        source_yield.reshape(2, blocks, 128),
        source_momentum.reshape(3, blocks, 128),
    )
    return gain.reshape(5, 1, 1, 1, gas_size)


def solution(mesh):
    sizes = (mesh.shape["gx"], mesh.shape["gy"], mesh.shape["gz"])
    in_specs = (
        P(None, "gx", "gy", "gz", None),
        P("gx", "gy", "gz", None),
        P(None, "gx", "gy", "gz", None),
        P("gx", "gy", "gz", None),
        P(None, "gx", "gy", "gz", None),
        P(None, "gx", "gy", "gz", None),
        P("gx", "gy", "gz", None, None),
        P("gx", "gy", "gz"),
    )
    out_specs = P(None, "gx", "gy", "gz", None)
    return jax.shard_map(
        functools.partial(local, sizes), mesh=mesh, in_specs=in_specs, out_specs=out_specs, check_vma=False
    )
```

```python
import functools
import math

import jax
import jax.numpy as jnp
from jax import lax
from jax.experimental import pallas as pl
from jax.experimental.pallas import tpu as pltpu
from jax.sharding import PartitionSpec as P


def kinds(count):
    return min(count, 3)


def kind_of(offset, count):
    if count >= 3:
        return offset + 1
    if count == 2:
        return jnp.abs(offset)
    return offset * 0


def own_kind(count):
    return 1 if count >= 3 else 0


def steps_of(count):
    if count >= 3:
        return ((0, -1), (2, 1))
    return ((1, 1),) if count == 2 else ()


MESH = pl.DeviceIdType.MESH
LIMIT = 67_043_328 - 64 * 1024


def shifted(axis, count, step):
    return lax.rem(lax.axis_index(axis) + step + count, count)


def columns_of(sizes):
    nx, ny, _ = sizes
    choices_x = steps_of(nx) + ((own_kind(nx), 0),)
    choices_y = ((own_kind(ny), 0),) + steps_of(ny)
    return [
        ((i, j), {"gx": shifted("gx", nx, dx), "gy": shifted("gy", ny, dy)})
        for i, dx in choices_x
        for j, dy in choices_y
        if dx or dy
    ]


def far_first(sizes):
    nx, ny, _ = sizes
    turn_x = 2 * lax.rem(lax.axis_index("gx"), 2) - 1
    turn_y = jnp.where(lax.axis_index("gy") == 0, -1, 1)
    choices_x = [(1 + turn_x, turn_x), (1 - turn_x, -turn_x)] if nx >= 3 else list(steps_of(nx))
    choices_y = [(1 + turn_y, turn_y), (1 - turn_y, -turn_y)] if ny >= 3 else list(steps_of(ny))
    own_x, own_y = (own_kind(nx), 0), (own_kind(ny), 0)
    order = [(x, y) for y in choices_y for x in choices_x + [own_x]] + [(x, own_y) for x in choices_x]
    return [((i, j), {"gx": shifted("gx", nx, dx), "gy": shifted("gy", ny, dy)}) for (i, dx), (j, dy) in order]


def far_roles(sizes):
    steps_x, steps_y = len(steps_of(sizes[0])), len(steps_of(sizes[1]))
    return ([3] * steps_x + [1]) * steps_y + [2] * steps_x


def facing_at(kind, count):
    return 2 - kind if count >= 3 else kind


def cores_of(sizes):
    return [(k, {"gz": shifted("gz", sizes[2], dz)}) for k, dz in steps_of(sizes[2])]


def greet(sizes, meanwhile):
    barrier = pltpu.get_barrier_semaphore()
    own = (own_kind(sizes[0]), own_kind(sizes[1]))
    peers = [c for c in columns_of(sizes) if c[0][0] == own[0] or c[0][1] == own[1]] + cores_of(sizes)
    for _, device in peers:
        pl.semaphore_signal(barrier, inc=1, device_id=device, device_id_type=MESH)
    meanwhile()
    if peers:
        pl.semaphore_wait(barrier, len(peers))


def facing(kind, count):
    return 2 - kind if count >= 3 else kind


PARTS = 16


def split3(value):
    first = value.astype(jnp.bfloat16).astype(jnp.float32)
    rest = value - first
    second = rest.astype(jnp.bfloat16).astype(jnp.float32)
    return first, second, rest - second


def offsets():
    return [(a, b, c) for a in (-1, 0, 1) for b in (-1, 0, 1) for c in (-1, 0, 1)]


def kind_at(offset, count):
    if count >= 3:
        return offset + 1
    return abs(offset) if count == 2 else 0


def place_at(offset, sizes):
    i, j, k = (kind_at(o, n) for o, n in zip(offset, sizes))
    return (i * kinds(sizes[1]) + j) * kinds(sizes[2]) + k


def role_places(role, sizes):
    places = [place_at(o, sizes) for o in offsets() if (o[0] != 0, o[1] != 0) == (role >= 2, role % 2 == 1)]
    return sorted(set(places))


def role_slots(role):
    return [n for n, o in enumerate(offsets()) if (o[0] != 0, o[1] != 0) == (role >= 2, role % 2 == 1)]


def gas_features(gas, feat, slot, offset):
    tiles = gas[3].shape[0]
    px, py, pz = (gas[k] + (offset[k] - 0.5) for k in range(3))
    root = lax.rsqrt(gas[3])
    square = (px * px + py * py + pz * pz) * root
    base = [n for role in range(4) for n in role_slots(role)].index(slot) * tiles
    for comp, value in enumerate((px * root, py * root, pz * root, square, root)):
        for part, piece in enumerate(split3(value)):
            at = (part * 5 + comp) * 128
            feat[base : base + tiles, at : at + 128] = piece.astype(jnp.bfloat16)


def source_features(pos, radius, rows, left):
    blocks = pos.shape[1]
    r = radius[...]
    inv = 1.0 / (r * r)
    sx, sy, sz = (pos[k] - 0.5 for k in range(3))
    comps = [-2.0 * inv * sx, -2.0 * inv * sy, -2.0 * inv * sz, inv, 1.0 + inv * (sx * sx + sy * sy + sz * sz)]
    parts = [split3(v) for v in comps]
    zero = jnp.zeros_like(r)
    for group in range(3):
        for part in range(3):
            for comp in range(5):
                value = parts[comp][group] if part + group < 3 else zero
                rows[pl.ds(group * PARTS + part * 5 + comp, blocks, stride=3 * PARTS), :] = value
        rows[pl.ds(group * PARTS + 15, blocks, stride=3 * PARTS), :] = zero
    for b in range(blocks):
        left[b] = rows[b * 3 * PARTS : (b + 1) * 3 * PARTS, :].T.astype(jnp.bfloat16)


def over_blocks(blocks, unroll, body):
    def step(i, carry):
        for k in range(unroll):
            body(i * unroll + k)
        return carry

    lax.fori_loop(0, blocks // unroll, step, 0)


def gather(role, tiles, feat, hot_in, picked):
    slots = [n for r in range(4) for n in role_slots(r)]
    first = slots.index(role_slots(role)[0]) * tiles
    depth = len(role_slots(role)) * tiles
    pairs = hot_in.shape[1]
    got = jnp.dot(hot_in[role, :, 0:depth], feat[first : first + depth, :], preferred_element_type=jnp.float32)
    for row in range(PARTS - 1):
        picked[role, pl.ds(row, pairs, stride=PARTS), :] = got[:, row * 128 : row * 128 + 128]


def weigh(role, picked, left, weights, sums, norms, unroll):
    blocks = left.shape[0]

    def body(b):
        near = []
        for z in range(2):
            at = pl.multiple_of((z * blocks + b) * PARTS, PARTS)
            near.append(picked[role, pl.ds(at, PARTS), :].astype(jnp.bfloat16))
        rhs = jnp.concatenate([jnp.concatenate(near, axis=1)] * 3, axis=0)
        u = jnp.dot(left[b], rhs, preferred_element_type=jnp.float32)
        w = 1.0 / (u * u)
        part = w[:, :128] + w[:, 128:]
        if role:
            part = sums[b] + part
        if role < 3:
            sums[b] = part
        else:
            norms[pl.ds(b, 1), :] = jnp.sum(part.T, axis=0, keepdims=True)
        w1 = w.astype(jnp.bfloat16)
        weights[role, b, 0:128] = w1
        weights[role, b, 128:256] = (w - w1.astype(jnp.float32)).astype(jnp.bfloat16)

    over_blocks(blocks, unroll, body)


def normalise(count, norms, yields, momentum, loads):
    blocks = norms.shape[0]
    lane = lax.broadcasted_iota(jnp.int32, (blocks, 128), 1)
    index = lax.broadcasted_iota(jnp.int32, (blocks, 128), 0) * 128 + lane
    scale = jnp.where(index < count[0, 0], 1.0, 0.0) / norms[...]
    for q, value in enumerate([yields[0], momentum[0], momentum[1], momentum[2], yields[1]]):
        coef = value * scale
        high = coef.astype(jnp.bfloat16).astype(jnp.float32)
        loads[pl.ds(q, blocks, stride=16), :] = high
        loads[pl.ds(q + 8, blocks, stride=16), :] = coef - high


def deposit(role, loads, weights, moved, unroll):
    blocks = weights.shape[1]

    def body(b):
        half = loads[pl.ds(pl.multiple_of(b * 16, 16), 16), :].astype(jnp.bfloat16)
        got = jnp.dot(jnp.concatenate([half, half], axis=1), weights[role, b], preferred_element_type=jnp.float32)
        both = got[0:8] + got[8:16]
        for z in range(2):
            start = pl.multiple_of((z * blocks + b) * 8, 8)
            moved[role, pl.ds(start, 8), :] = both[:, z * 128 : z * 128 + 128]

    over_blocks(blocks, unroll, body)


def one_hots(sizes, tiles, table_rows, hot_in, hot_out):
    nx, ny, nz = sizes
    ids = table_rows[...]
    slot, tile = ids // tiles, ids % tiles
    at = kind_of(slot // 9 - 1, nx) * kinds(ny) + kind_of(slot // 3 % 3 - 1, ny)
    at = (at * kinds(nz) + kind_of(slot % 3 - 1, nz)) * tiles + tile
    flip_a = slot[0:1] // 9 == 0
    flip_b = slot[0:1] // 3 % 3 == 0

    def pick(values, role):
        row = []
        for z in range(2):
            low, high = (
                jnp.where(flip_b, values[4 * a + z + 2 : 4 * a + z + 3], values[4 * a + z : 4 * a + z + 1])
                if role % 2 == 0
                else jnp.where(flip_b, values[4 * a + z : 4 * a + z + 1], values[4 * a + z + 2 : 4 * a + z + 3])
                for a in range(2)
            )
            row.append(jnp.where(flip_a, high, low) if role < 2 else jnp.where(flip_a, low, high))
        return jnp.concatenate(row, axis=1)

    for role in range(4):
        source, target = pick(ids, role), pick(at, role)
        pairs = source.shape[1]
        index = lax.broadcasted_iota(jnp.int32, (tiles, pairs), 0)
        hot = [(index + n * tiles == source).astype(jnp.float32) for n in role_slots(role)]
        depth = len(hot) * tiles
        hot_in[role, :, 0:depth] = jnp.concatenate(hot, axis=0).T.astype(jnp.bfloat16)
        hot = [(index + n * tiles == target).astype(jnp.float32) for n in role_places(role, sizes)]
        hot = jnp.concatenate(hot, axis=0).astype(jnp.bfloat16)
        hot_out[role, 0 : hot.shape[0], :] = jnp.concatenate([hot, hot], axis=1)


def scatter(role, sizes, hot_out, moved, out, done):
    tiles = out.shape[2]
    places = role_places(role, sizes)
    pairs = hot_out.shape[2] // 2
    values = jnp.concatenate([moved[role, pl.ds(q, pairs, stride=8), :] for q in range(5)], axis=1)
    m1 = values.astype(jnp.bfloat16)
    m2 = (values - m1.astype(jnp.float32)).astype(jnp.bfloat16)
    hot = hot_out[role, 0 : len(places) * tiles, :]
    got = jnp.dot(hot, jnp.concatenate([m1, m2], axis=0), preferred_element_type=jnp.float32)
    for n, place in enumerate(places):
        for q in range(5):
            value = got[n * tiles : (n + 1) * tiles, q * 128 : (q + 1) * 128]
            out[place, q] = out[place, q] + value if place in done else value
        done.add(place)


def core_scratch(blocks, tiles):
    return [
        pltpu.VMEM((27 * tiles, (PARTS - 1) * 128), jnp.bfloat16),
        pltpu.VMEM((blocks * 3 * PARTS, 128), jnp.float32),
        pltpu.VMEM((blocks, 128, 3 * PARTS), jnp.bfloat16),
        pltpu.VMEM((4, blocks, 256, 256), jnp.bfloat16),
        pltpu.VMEM((blocks, 128, 128), jnp.float32),
        pltpu.VMEM((blocks, 128), jnp.float32),
        pltpu.VMEM((blocks * 16, 128), jnp.float32),
        pltpu.VMEM((4, blocks * 16, 128), jnp.float32),
        pltpu.VMEM((4, 2 * blocks, 12 * tiles), jnp.bfloat16),
        pltpu.VMEM((4, 12 * tiles, 4 * blocks), jnp.bfloat16),
        pltpu.VMEM((4, 2 * blocks * PARTS, 128), jnp.float32),
    ]


def fused_kernel(sizes, pos, mass, table, count, spos, sradius, syield, smomentum, out, *scratch):
    (near, count_s, table_v, pos_v, radius_v, yield_v, momentum_v, deposits, part, got_z, got) = scratch[:11]
    (feat, rows, left, weights, sums, norms, loads, moved, hot_in, hot_out, picked) = scratch[11:22]
    local_sem, send_sem, recv_sem, gsend_z, grecv_z, gsend, grecv, ready_sem = scratch[22:]
    nx, ny, nz = sizes
    own = tuple(own_kind(n) for n in sizes)
    tiles = near.shape[2]
    blocks = pos_v.shape[1]
    unroll = math.gcd(blocks, 16)

    def place(i, j, k):
        return (i * kinds(ny) + j) * kinds(nz) + k

    home = place(*own)
    gas_in = [
        pltpu.make_async_copy(pos, near.at[home, pl.ds(0, 3)], local_sem.at[0]),
        pltpu.make_async_copy(mass, near.at[home, pl.ds(3, 1)], local_sem.at[1]),
    ]
    pairs = [(spos, pos_v), (sradius, radius_v), (syield, yield_v), (smomentum, momentum_v)]
    pairs += [(count, count_s), (table, table_v)]
    rest_in = [pltpu.make_async_copy(src, dst, local_sem.at[2 + n]) for n, (src, dst) in enumerate(pairs)]
    for copy in gas_in + rest_in:
        copy.start()

    def features(i, j, k):
        gas = [near[place(i, j, k), c] for c in range(4)]
        for slot, offset in enumerate(offsets()):
            if place_at(offset, sizes) == place(i, j, k):
                gas_features(gas, feat, slot, offset)

    def meanwhile():
        for copy in gas_in + rest_in:
            copy.wait()
        source_features(pos_v, radius_v, rows, left)
        one_hots(sizes, tiles, table_v, hot_in, hot_out)
        loads[...] = jnp.zeros_like(loads)
        spare = jnp.zeros((2 * blocks, 128), jnp.float32)
        for side in range(4):
            picked[side, pl.ds(PARTS - 1, 2 * blocks, stride=PARTS), :] = spare
        features(*own)

    greet(sizes, meanwhile)
    finished = []

    def gas_copy(source, target, device):
        return pltpu.make_async_remote_copy(
            src_ref=near.at[source],
            dst_ref=near.at[target],
            send_sem=send_sem.at[target],
            recv_sem=recv_sem.at[target],
            device_id=device,
            device_id_type=MESH,
        )

    def send(source, target, device):
        copy = gas_copy(source, target, device)
        copy.start()
        finished.append(copy)

    def arrived(i, j, k):
        target = place(i, j, k)
        gas_copy(target, target, next(iter(cores_of(sizes) + columns_of(sizes)))[1]).wait_recv()

    def to_cores(i, j):
        for k, device in cores_of(sizes):
            send(place(i, j, own[2]), place(i, j, facing(k, nz)), device)

    columns = columns_of(sizes)
    far = list(zip(far_first(sizes), far_roles(sizes)))
    others = [device for at, device in columns if at[0] != own[0] and at[1] == own[1]]
    corners = [device for at, device in columns if at[0] != own[0] and at[1] != own[1]]
    if corners:
        for device in others:
            pl.semaphore_signal(ready_sem, inc=1, device_id=device, device_id_type=MESH)

    def send_home(roles):
        for ((i, j), device), role in far:
            if role in roles:
                send(home, place(facing_at(i, nx), facing_at(j, ny), own[2]), device)

    def ready():
        if corners:
            pl.semaphore_wait(ready_sem, len(others))
        send_home((3,))

    send_home((1, 2))
    to_cores(own[0], own[1])

    def weigh_role(role):
        gather(role, tiles, feat, hot_in, picked)
        weigh(role, picked, left, weights, sums, norms, unroll)

    def sides(role):
        return [at for at, _ in columns if 2 * (at[0] != own[0]) + (at[1] != own[1]) == role]

    def take(role):
        for at in sides(role):
            arrived(at[0], at[1], own[2])
            to_cores(*at)
            pass

    def early(role):
        for at in sides(role):
            features(at[0], at[1], own[2])

    def finish(role):
        for i, j in sides(role):
            for k, _ in steps_of(nz):
                arrived(i, j, k)
                features(i, j, k)
        weigh_role(role)

    def received(role):
        for i, j in sides(role):
            for k, _ in steps_of(nz):
                arrived(i, j, k)
                features(i, j, k)

    def pick(role):
        gather(role, tiles, feat, hot_in, picked)

    def weight(role):
        weigh(role, picked, left, weights, sums, norms, unroll)

    ready()
    for k, _ in steps_of(nz):
        arrived(own[0], own[1], k)
        features(own[0], own[1], k)
    pick(0)
    weight(0)
    take(1)
    take(2)
    early(1)
    early(2)
    received(1)
    pick(1)
    received(2)
    pick(2)
    weight(1)
    weight(2)
    take(3)
    early(3)
    received(3)
    pick(3)
    weight(3)
    normalise(count_s, norms, yield_v, momentum_v, loads)
    done = set()

    def gain_copy(src, dst, send_at, recv_at, device):
        return pltpu.make_async_remote_copy(
            src_ref=src, dst_ref=dst, send_sem=send_at, recv_sem=recv_at, device_id=device, device_id_type=MESH
        )

    def z_copy(i, j, k, device):
        at = place(i, j, k)
        return gain_copy(deposits.at[at], got_z.at[at], gsend_z.at[at], grecv_z.at[at], device)

    def side_copy(i, j, device):
        at = i * kinds(ny) + j
        return gain_copy(part.at[at], got.at[at], gsend.at[at], grecv.at[at], device)

    def start(copy):
        copy.start()
        finished.append(copy)

    def column_total(i, j):
        total = deposits[place(i, j, own[2])]
        for k, device in cores_of(sizes):
            z_copy(i, j, k, device).wait_recv()
            total = total + got_z[place(i, j, k)]
        return total

    def role_columns(role):
        return [c for c, r in far if r == role]

    waiting = []

    def flush():
        while waiting:
            start(waiting.pop(0))

    def totals(role):
        for (i, j), device in role_columns(role):
            part[i * kinds(ny) + j] = column_total(i, j)
            flush()
            waiting.append(side_copy(i, j, device))

    for role in (3, 2, 1, 0):
        deposit(role, loads, weights, moved, unroll)
        flush()
        scatter(role, sizes, hot_out, moved, deposits, done)
        for (i, j), _ in role_columns(role) if role else [(own[:2], None)]:
            for k, device in cores_of(sizes):
                start(z_copy(i, j, k, device))
        if role < 3:
            totals(role + 1)
    flush()
    total = column_total(*own[:2])
    for (i, j), device in columns:
        side_copy(i, j, device).wait_recv()
        total = total + got[i * kinds(ny) + j]
    out[...] = total / near[home, 3]
    for copy in finished:
        copy.wait_send()


def local(sizes, gas_pos, gas_mass, source_pos, source_radius, source_yield, source_momentum, source_tiles, source_count):
    gas_size = gas_pos.shape[-1]
    tiles = gas_size // 128
    blocks = source_pos.shape[-1] // 128
    listed = source_tiles.shape[-1]
    slots = kinds(sizes[0]) * kinds(sizes[1]) * kinds(sizes[2])
    sides = kinds(sizes[0]) * kinds(sizes[1])
    piece = (5, tiles, 128)
    given = pl.BlockSpec(memory_space=pltpu.HBM)
    dma = pltpu.SemaphoreType.DMA
    gain = pl.pallas_call(
        functools.partial(fused_kernel, sizes),
        out_shape=pltpu.VMEM(piece, jnp.float32),
        in_specs=[given] * 8,
        out_specs=pl.BlockSpec(memory_space=pltpu.VMEM),
        scratch_shapes=[
            pltpu.VMEM((slots, 4, tiles, 128), jnp.float32),
            pltpu.SMEM((1, 1), jnp.int32),
            pltpu.VMEM((listed, blocks), jnp.int32),
            pltpu.VMEM((3, blocks, 128), jnp.float32),
            pltpu.VMEM((blocks, 128), jnp.float32),
            pltpu.VMEM((2, blocks, 128), jnp.float32),
            pltpu.VMEM((3, blocks, 128), jnp.float32),
            pltpu.VMEM((slots, *piece), jnp.float32),
            pltpu.VMEM((sides, *piece), jnp.float32),
            pltpu.VMEM((slots, *piece), jnp.float32),
            pltpu.VMEM((sides, *piece), jnp.float32),
            *core_scratch(blocks, tiles),
            dma((8,)),
            dma((slots,)),
            dma((slots,)),
            dma((slots,)),
            dma((slots,)),
            dma((sides,)),
            dma((sides,)),
            pltpu.SemaphoreType.REGULAR,
        ],
        compiler_params=pltpu.CompilerParams(collective_id=0, has_side_effects=True, vmem_limit_bytes=LIMIT),
    )(
        gas_pos.reshape(3, tiles, 128),
        gas_mass.reshape(1, tiles, 128),
        source_tiles.reshape(blocks, listed).T,
        source_count.reshape(1, 1),
        source_pos.reshape(3, blocks, 128),
        source_radius.reshape(blocks, 128),
        source_yield.reshape(2, blocks, 128),
        source_momentum.reshape(3, blocks, 128),
    )
    return gain.reshape(5, 1, 1, 1, gas_size)


def solution(mesh):
    sizes = (mesh.shape["gx"], mesh.shape["gy"], mesh.shape["gz"])
    in_specs = (
        P(None, "gx", "gy", "gz", None),
        P("gx", "gy", "gz", None),
        P(None, "gx", "gy", "gz", None),
        P("gx", "gy", "gz", None),
        P(None, "gx", "gy", "gz", None),
        P(None, "gx", "gy", "gz", None),
        P("gx", "gy", "gz", None, None),
        P("gx", "gy", "gz"),
    )
    out_specs = P(None, "gx", "gy", "gz", None)
    return jax.shard_map(
        functools.partial(local, sizes), mesh=mesh, in_specs=in_specs, out_specs=out_specs, check_vma=False
    )
```
